8 devices in a mesh: dp: 1 (over z), tp: 8 (over y, x, core).
Axes of the slice: x: 2, y: 2, z: 1, core: 2. Of those that a mesh axis runs over, the one named last changes fastest.
Arguments:
- residual: bfloat16 [512, 1152], P('dp', 'tp')
- lengths: int32 [512], P(('dp', 'tp'))
- ln_scale: bfloat16 [2, 1152], P(None, 'tp')
- w_in: bfloat16 [2, 1152, 14848], P(None, None, 'tp')
- w_key: bfloat16 [2, 1152, 256], replicated
- w_val: bfloat16 [2, 1152, 256], replicated
- w_out: bfloat16 [2, 7936, 1152], P(None, 'tp')
- key_cache: bfloat16 [2, 512, 256, 256], P(None, ('dp', 'tp'))
- val_cache: bfloat16 [2, 512, 256, 256], P(None, ('dp', 'tp'))
Outputs:
- output 1: bfloat16 [512, 1152], P('dp', 'tp')
- output 2: bfloat16 [2, 512, 256, 256], P(None, ('dp', 'tp'))
- output 3: bfloat16 [2, 512, 256, 256], P(None, ('dp', 'tp'))
All inputs are finite; a program needn't handle non-finite values.
Results may differ from the reference program's by a relative error of at most 0.0118485.
Values are sent between devices in bfloat16 or wider.
A program may use at most 1 GiB of HBM per device.

```python
import math
import jax
import jax.numpy as jnp
from jax import lax

WIDTH = 1152
FFN_WIDTH = 6912
HEADS = 4
HEAD_DIM = 256
TP_SIZE = 8
BATCH = 512
CACHE_LEN = 256

Q_WIDTH = HEADS * HEAD_DIM
FFN_DEV = FFN_WIDTH // TP_SIZE
Q_DEV = Q_WIDTH // TP_SIZE
CACHE_BITS = int(math.log2(CACHE_LEN))


def setup_inputs(seed: int = 0, part: int = 0) -> dict:
    base_key = jax.random.key(seed)
    root_keys = jax.random.split(base_key, 2)
    shared_keys = jax.random.split(root_keys[0], 5)
    part_root = jax.random.fold_in(root_keys[1], part)
    own_keys = jax.random.split(part_root, 5)
    length_keys = jax.random.split(jax.random.fold_in(part_root, 1), 3)
    col_pos = jnp.arange(WIDTH, dtype=jnp.float32) * (2.0 / WIDTH) - 1.0
    noise = jax.random.normal(own_keys[0], (BATCH, WIDTH), jnp.float32)
    slopes = 1.5 * jax.random.normal(own_keys[1], (BATCH, 1), jnp.float32)
    offsets = jax.random.normal(own_keys[2], (BATCH, 1), jnp.float32)
    residual = (noise + slopes * col_pos[None, :] + offsets).astype(jnp.bfloat16)
    shifts = jax.random.randint(length_keys[0], (BATCH,), 0, CACHE_BITS + 1)
    uppers = jnp.minimum(jnp.power(2, shifts), CACHE_LEN)
    lengths = jax.random.randint(length_keys[1], (BATCH,), 0, uppers)
    longest = jax.random.randint(length_keys[2], (), 0, BATCH)
    lengths = jnp.where(jnp.arange(BATCH) == longest, CACHE_LEN - 1, lengths).astype(jnp.int32)
    cache_shape = (2, BATCH, CACHE_LEN, HEAD_DIM)
    key_cache = jax.random.normal(own_keys[3], cache_shape, jnp.float32).astype(jnp.bfloat16)
    val_cache = jax.random.normal(own_keys[4], cache_shape, jnp.float32).astype(jnp.bfloat16)
    in_scale = WIDTH ** -0.5
    out_scale = (FFN_WIDTH + Q_WIDTH) ** -0.5
    ln_scale = (1.0 + 0.3 * jax.random.normal(shared_keys[0], (2, WIDTH), jnp.float32)).astype(jnp.bfloat16)
    w_in = (in_scale * jax.random.normal(shared_keys[1], (2, WIDTH, 2 * FFN_WIDTH + Q_WIDTH), jnp.float32)).astype(jnp.bfloat16)
    w_key = (in_scale * jax.random.normal(shared_keys[2], (2, WIDTH, HEAD_DIM), jnp.float32)).astype(jnp.bfloat16)
    w_val = (in_scale * jax.random.normal(shared_keys[3], (2, WIDTH, HEAD_DIM), jnp.float32)).astype(jnp.bfloat16)
    w_out = (out_scale * jax.random.normal(shared_keys[4], (2, FFN_WIDTH + Q_WIDTH, WIDTH), jnp.float32)).astype(jnp.bfloat16)
    return {"residual": residual, "lengths": lengths, "ln_scale": ln_scale, "w_in": w_in, "w_key": w_key, "w_val": w_val, "w_out": w_out, "key_cache": key_cache, "val_cache": val_cache}


def layer_norm(resid_in, ln_row):
    resid_f32 = resid_in.astype(jnp.float32)
    row_mean = jnp.sum(resid_f32, axis=-1, keepdims=True) / WIDTH
    row_var = jnp.sum(resid_f32 * resid_f32, axis=-1, keepdims=True) / WIDTH - row_mean * row_mean
    return ((resid_f32 - row_mean) * lax.rsqrt(row_var + 1e-6) * ln_row.astype(jnp.float32)).astype(jnp.bfloat16)


def rotary(vectors, angles):
    half_dim = vectors.shape[-1] // 2
    first_half = vectors[..., :half_dim].astype(jnp.float32)
    second_half = vectors[..., half_dim:].astype(jnp.float32)
    cos_part = jnp.cos(angles)
    sin_part = jnp.sin(angles)
    return jnp.concatenate([first_half * cos_part - second_half * sin_part, second_half * cos_part + first_half * sin_part], axis=-1).astype(jnp.bfloat16)


def reference(residual, lengths, ln_scale, w_in, w_key, w_val, w_out, key_cache, val_cache):
    inv_freq = 10000.0 ** (-jnp.arange(HEAD_DIM // 2, dtype=jnp.float32) * (2.0 / HEAD_DIM))
    angles = lengths.astype(jnp.float32)[:, None] * inv_freq[None, :]
    positions = jnp.arange(CACHE_LEN)
    slot_mask = positions[None, :, None] == lengths[:, None, None]
    visible = positions[None, None, :] <= lengths[:, None, None]

    def one_layer(resid_in, layer_params):
        ln_row, w_in_layer, w_key_layer, w_val_layer, w_out_layer, key_layer, val_layer = layer_params
        normed = layer_norm(resid_in, ln_row)
        fused_out = jnp.dot(normed, w_in_layer, preferred_element_type=jnp.float32).astype(jnp.bfloat16).reshape(BATCH, TP_SIZE, 2 * FFN_DEV + Q_DEV)
        gate_vals = fused_out[:, :, :FFN_DEV].astype(jnp.float32)
        up_vals = fused_out[:, :, FFN_DEV:2 * FFN_DEV].astype(jnp.float32)
        activated = (jax.nn.silu(gate_vals) * up_vals).astype(jnp.bfloat16)
        query_rows = rotary(fused_out[:, :, 2 * FFN_DEV:].reshape(BATCH, HEADS, HEAD_DIM), angles[:, None, :])
        new_key = rotary(jnp.dot(normed, w_key_layer, preferred_element_type=jnp.float32).astype(jnp.bfloat16), angles)
        new_val = jnp.dot(normed, w_val_layer, preferred_element_type=jnp.float32).astype(jnp.bfloat16)
        key_new_cache = jnp.where(slot_mask, new_key[:, None, :], key_layer)
        val_new_cache = jnp.where(slot_mask, new_val[:, None, :], val_layer)
        scores = jnp.einsum("bhd,bsd->bhs", query_rows.astype(jnp.float32), key_new_cache.astype(jnp.float32)) * HEAD_DIM ** -0.5
        scores = jnp.where(visible, scores, -1e30)
        weights = jnp.exp(scores - jnp.max(scores, axis=-1, keepdims=True))
        weight_sum = jnp.sum(weights, axis=-1, keepdims=True)
        mixed_vals = jnp.einsum("bhs,bsd->bhd", weights.astype(jnp.bfloat16).astype(jnp.float32), val_new_cache.astype(jnp.float32)) / weight_sum
        attn_cols = mixed_vals.astype(jnp.bfloat16).reshape(BATCH, TP_SIZE, Q_DEV)
        joined = jnp.concatenate([activated, attn_cols], axis=2).reshape(BATCH, FFN_WIDTH + Q_WIDTH)
        update = jnp.dot(joined, w_out_layer, preferred_element_type=jnp.float32)
        resid_out = (resid_in.astype(jnp.float32) + update).astype(jnp.bfloat16)
        return resid_out, (key_new_cache, val_new_cache)

    resid_final, cache_pair = lax.scan(one_layer, residual, (ln_scale, w_in, w_key, w_val, w_out, key_cache, val_cache))
    return resid_final, cache_pair[0], cache_pair[1]
```

```python
import functools

import jax
import jax.numpy as jnp
import numpy as np
from jax import lax
from jax.experimental import pallas as pl
from jax.experimental.pallas import tpu as pltpu
from jax.sharding import PartitionSpec as P

NORM_EPS = 1e-6
MESH = pl.DeviceIdType.MESH
CHUNKS = 2
BF = jnp.bfloat16
F32 = jnp.float32
TN = (((0,), (0,)), ((), ()))
NT = (((1,), (1,)), ((), ()))


def dot(a, b, dims=None):
    if dims is None:
        return jnp.dot(a, b, preferred_element_type=F32)
    return lax.dot_general(a, b, dims, preferred_element_type=F32)


def iota2(shape, dim):
    return lax.broadcasted_iota(jnp.int32, shape, dim)


def step_kernel(r_in, len_row, ln_in, inv_freq, w_in, w_key, w_val, w_out, k_cache, v_cache,
                r_out, new_k, new_v,
                w_in_v, w_key_v, w_val_v, w_out_v, k_buf, v_buf,
                r_all, ln_all, ln_col, h_t, joined, y_part, d2d, rs_recv, rs_send,
                q_send, q_recv, o_send, o_recv, q_rows, s_rows, o_rows, kv_tmp,
                cos_b, sin_b, len_col, len_rep, perm,
                w_sems, c_sems, ln_ss, ln_rs, ag_ss, ag_rs, q_ss, q_rs, o_ss, o_rs, d_ss, d_rs, t_ss, t_rs):
    layers, width = w_in.shape[0], w_in.shape[2]
    shard, batch = r_in.shape
    tp = width // shard
    rows = batch // tp
    q_dev = q_send.shape[2]
    ffn_dev = w_out.shape[1] - q_dev
    head_dim = w_key.shape[2]
    half = head_dim // 2
    heads = q_dev * tp // head_dim
    cw = batch // CHUNKS
    hw = cw // 2
    cr = rows // CHUNKS
    hr = cr * heads

    me = lax.axis_index("tp")
    core, xpos, ypos = me % 2, (me // 2) % 2, me // 4
    dp_ = me + 1 - 2 * core
    dx = me + 2 - 4 * xpos
    dy = me + 4 - 8 * ypos
    dd = dx + 4 - 8 * ypos
    flip = 1 - 2 * core

    def rcopy(src, dst, ss, rs, dev):
        return pltpu.make_async_remote_copy(src_ref=src, dst_ref=dst, send_sem=ss, recv_sem=rs,
                                            device_id={"tp": dev}, device_id_type=MESH)

    barrier = pltpu.get_barrier_semaphore()
    for off in range(1, tp):
        pl.semaphore_signal(barrier, 1, device_id={"tp": (me + off) % tp}, device_id_type=MESH)

    loads = {}

    def load(name, src, dst, sem):
        loads[name] = pltpu.make_async_copy(src, dst, sem)
        loads[name].start()

    def load_weights(l):
        load(("in", l), w_in.at[l], w_in_v.at[l], w_sems.at[l, 0])
        load(("key", l), w_key.at[l], w_key_v.at[l], w_sems.at[l, 1])
        load(("val", l), w_val.at[l], w_val_v.at[l], w_sems.at[l, 2])
        load(("out", l), w_out.at[l], w_out_v.at[l], w_sems.at[l, 3])

    def load_cache(l, c):
        load(("k", l, c), k_cache.at[l, pl.ds(c * cr, cr)], k_buf.at[pl.ds(c * cr, cr)], c_sems.at[l, c, 0])
        load(("v", l, c), v_cache.at[l, pl.ds(c * cr, cr)], v_buf.at[pl.ds(c * cr, cr)], c_sems.at[l, c, 1])

    load_weights(0)
    load_cache(0, 0)
    load_cache(0, 1)

    src_i = iota2((batch, batch), 0)
    dst_i = iota2((batch, batch), 1)
    want = ((dst_i % cw) // cr) * rows + (dst_i // cw) * cr + dst_i % cr
    perm[...] = jnp.where(src_i == want, 1.0, 0.0).astype(BF)
    r_all[0, me] = dot(r_in[...], perm[...]).astype(BF)
    ln_all[me] = ln_in[...]

    pl.semaphore_wait(barrier, tp - 1)

    sends = []

    def lanes(c, h):
        return pl.ds(c * cw + h * hw, hw)

    def ag_send(l, c, idx, dev, slot, h):
        ref = r_all.at[l, slot, :, lanes(c, h)]
        cp = rcopy(ref, ref, ag_ss.at[l, c, idx], ag_rs.at[l, c, slot, h], dev)
        cp.start()
        sends.append(cp)

    def ag_wait(l, c, slot, h):
        ref = r_all.at[l, slot, :, lanes(c, h)]
        rcopy(ref, ref, ag_ss.at[l, c, 0], ag_rs.at[l, c, slot, h], dp_).wait_recv()

    def ag_start(l, c):
        ag_send(l, c, 0, dx, me, 0)
        ag_send(l, c, 1, dy, me, 1)
        ag_send(l, c, 2, dx, me, 1)
        ag_send(l, c, 3, dy, me, 0)
        ag_send(l, c, 4, dp_, me, 0)
        ag_send(l, c, 5, dp_, me, 1)

    def ag_forward(l, c):
        ag_wait(l, c, dx, 0)
        ag_send(l, c, 6, dy, dx, 0)
        ag_send(l, c, 7, dp_, dx, 0)
        ag_wait(l, c, dy, 1)
        ag_send(l, c, 8, dx, dy, 1)
        ag_send(l, c, 9, dp_, dy, 1)

    def ag_relay(l, c):
        ag_wait(l, c, dx, 1)
        ag_send(l, c, 10, dp_, dx, 1)
        ag_wait(l, c, dy, 0)
        ag_send(l, c, 11, dp_, dy, 0)

    def ag_finish(l, c):
        ag_wait(l, c, dd, 0)
        ag_send(l, c, 12, dp_, dd, 0)
        ag_wait(l, c, dd, 1)
        ag_send(l, c, 13, dp_, dd, 1)
        for slot in (dp_, dx + flip, dy + flip, dd + flip):
            for h in (0, 1):
                ag_wait(l, c, slot, h)

    def ln_start():
        for off in range(1, tp):
            cp = rcopy(ln_all.at[me], ln_all.at[me], ln_ss.at[off - 1], ln_rs.at[off - 1], (me + off) % tp)
            cp.start()
            sends.append(cp)

    def ln_finish():
        for off in range(1, tp):
            ref = ln_all.at[(me + tp - off) % tp]
            rcopy(ref, ref, ln_ss.at[off - 1], ln_rs.at[off - 1], dp_).wait_recv()
        for l in range(layers):
            pick = jnp.where(iota2((layers, 128), 0) == l, 1.0, 0.0).astype(BF)
            for s in range(tp):
                ln_col[l, s] = dot(ln_all[s], pick, TN)

    def setup_angles():
        lens = len_row[...].astype(F32)
        for c in range(CHUNKS):
            own = iota2((cr, rows), 1) == iota2((cr, rows), 0) + c * cr
            lc = jnp.sum(jnp.where(own, lens, 0.0), axis=1, keepdims=True)
            len_col[c] = lc
            rep = iota2((hr, rows), 1) == iota2((hr, rows), 0) // heads + c * cr
            len_rep[c] = jnp.sum(jnp.where(rep, lens, 0.0), axis=1, keepdims=True)
            ang = lc * inv_freq[...]
            cos_b[c] = jnp.cos(ang)
            sin_b[c] = jnp.sin(ang)

    def norm_query(l, c):
        cl = pl.ds(c * cw, cw)
        total = jnp.zeros((shard, cw), F32)
        squares = jnp.zeros((shard, cw), F32)
        for s in range(tp):
            v = r_all[l, s, :, cl].astype(F32)
            total = total + v
            squares = squares + v * v
        mean = jnp.sum(total, axis=0, keepdims=True) / width
        var = jnp.sum(squares, axis=0, keepdims=True) / width - mean * mean
        inv = lax.rsqrt(var + NORM_EPS)
        for s in range(tp):
            v = r_all[l, s, :, cl].astype(F32)
            scale = ln_col[l, s]
            scale = jnp.concatenate([scale] * (cw // 128), axis=1)
            h_t[pl.ds(s * shard, shard), cl] = ((v - mean) * inv * scale).astype(BF)
        q_t = dot(w_in_v[l, pl.ds(2 * ffn_dev, q_dev), :], h_t[:, cl])
        q_send[l, cl] = jnp.transpose(q_t).astype(BF)
        for off in range(1, tp):
            dev = (me + off) % tp
            cp = rcopy(q_send.at[l, pl.ds(c * cw + dev * cr, cr)], q_recv.at[l, c, me],
                       q_ss.at[l, c, off - 1], q_rs.at[l, c, off - 1], dev)
            cp.start()
            sends.append(cp)
        q_recv[l, c, me] = q_send[l, pl.ds(pl.multiple_of(c * cw + me * cr, cr), cr)]

    def key_value(l, c):
        per = 128 // cr
        blk = h_t[:, pl.ds(pl.multiple_of(c * cw + (me // per) * 128, 128), 128)]
        here = pl.ds(pl.multiple_of((me % per) * cr, cr), cr)
        kv_tmp[...] = dot(blk, w_key_v[l], TN)
        k = kv_tmp[here].astype(BF).astype(F32)
        x1, x2 = k[:, :half], k[:, half:]
        co, si = cos_b[c], sin_b[c]
        new_k[l, pl.ds(c * cr, cr), :half] = (x1 * co - x2 * si).astype(BF).astype(F32)
        new_k[l, pl.ds(c * cr, cr), half:] = (x2 * co + x1 * si).astype(BF).astype(F32)
        kv_tmp[...] = dot(blk, w_val_v[l], TN)
        new_v[l, pl.ds(c * cr, cr)] = kv_tmp[here].astype(BF).astype(F32)

    def feed_forward(l, c):
        cl = pl.ds(c * cw, cw)
        tile = 288

        def body(i, _):
            o = pl.multiple_of(i * tile, 32)
            gate = dot(w_in_v[l, pl.ds(o, tile)], h_t[:, cl]).astype(BF).astype(F32)
            up = dot(w_in_v[l, pl.ds(o + ffn_dev, tile)], h_t[:, cl]).astype(BF).astype(F32)
            joined[pl.ds(o, tile), cl] = (gate * jax.nn.sigmoid(gate) * up).astype(BF)
            return 0

        lax.fori_loop(0, ffn_dev // tile, body, 0)

    def attention(l, c):
        for off in range(1, tp):
            ref = q_recv.at[l, c, (me + tp - off) % tp]
            rcopy(ref, ref, q_ss.at[l, c, off - 1], q_rs.at[l, c, off - 1], dp_).wait_recv()
        co, si = cos_b[c], sin_b[c]
        r1, r2 = [], []
        for h in range(heads):
            x1 = q_recv[l, c, 2 * h].astype(F32)
            x2 = q_recv[l, c, 2 * h + 1].astype(F32)
            r1.append((x1 * co - x2 * si).astype(BF))
            r2.append((x2 * co + x1 * si).astype(BF))
        ri, ci = iota2((hr, hr), 0), iota2((hr, hr), 1)
        mix = jnp.where(ci == (ri % heads) * cr + ri // heads, 1.0, 0.0).astype(BF)
        q_rows[:, :half] = dot(mix, jnp.concatenate(r1, axis=0)).astype(BF)
        q_rows[:, half:] = dot(mix, jnp.concatenate(r2, axis=0)).astype(BF)
        rep = jnp.where(iota2((hr, cr), 1) == iota2((hr, cr), 0) // heads, 1.0, 0.0).astype(BF)
        k_rep = dot(rep, new_k[l, pl.ds(c * cr, cr)].astype(BF))
        v_rep = dot(rep, new_v[l, pl.ds(c * cr, cr)].astype(BF))
        q_all = q_rows[...].astype(F32)
        s_new = jnp.sum(q_all * k_rep, axis=1, keepdims=True) * head_dim ** -0.5
        group = 16 // heads
        which = iota2((16, head_dim), 0) // heads
        loads[("k", l, c)].wait()

        def score(g, _):
            o = pl.multiple_of(g * 16, 16)
            qg = q_rows[pl.ds(o, 16)]
            acc = jnp.zeros((16, head_dim), F32)
            for j in range(group):
                acc = jnp.where(which == j, dot(qg, k_buf[c * cr + g * group + j], NT), acc)
            s_rows[pl.ds(o, 16)] = acc
            return 0

        lax.fori_loop(0, hr // 16, score, 0, unroll=2)
        s = s_rows[...] * head_dim ** -0.5
        pos = iota2((hr, s.shape[1]), 1).astype(F32)
        s = jnp.where(pos < len_rep[c], s, -1e30)
        top = jnp.maximum(jnp.max(s, axis=1, keepdims=True), s_new)
        w = jnp.exp(s - top)
        w_new = jnp.exp(s_new - top)
        total = jnp.sum(w, axis=1, keepdims=True) + w_new
        q_rows[...] = w.astype(BF)
        loads[("v", l, c)].wait()

        def mixv(g, _):
            o = pl.multiple_of(g * 16, 16)
            wg = q_rows[pl.ds(o, 16)]
            acc = jnp.zeros((16, head_dim), F32)
            for j in range(group):
                acc = jnp.where(which == j, dot(wg, v_buf[c * cr + g * group + j]), acc)
            o_rows[pl.ds(o, 16)] = acc
            return 0

        lax.fori_loop(0, hr // 16, mixv, 0, unroll=2)
        mixed = (o_rows[...] + w_new.astype(BF).astype(F32) * v_rep) / total
        back = jnp.where(ri == (ci % heads) * cr + ci // heads, 1.0, 0.0).astype(BF)
        heads_o = dot(back, mixed.astype(BF)).astype(BF)
        for t in range(tp):
            o_send[l, c, t] = heads_o[(t // 2) * cr:(t // 2 + 1) * cr, (t % 2) * half:(t % 2 + 1) * half]
        for off in range(1, tp):
            dev = (me + off) % tp
            cp = rcopy(o_send.at[l, c, dev], o_recv.at[l, c, me], o_ss.at[l, c, off - 1], o_rs.at[l, c, off - 1], dev)
            cp.start()
            sends.append(cp)
        o_recv[l, c, me] = o_send[l, c, me]

    def project(l, c):
        cl = pl.ds(c * cw, cw)
        for off in range(1, tp):
            ref = o_recv.at[l, c, (me + tp - off) % tp]
            rcopy(ref, ref, o_ss.at[l, c, off - 1], o_rs.at[l, c, off - 1], dp_).wait_recv()
        o_all = jnp.concatenate([o_recv[l, c, j].astype(F32) for j in range(tp)], axis=0)
        joined[pl.ds(ffn_dev, q_dev), cl] = jnp.transpose(o_all).astype(BF)

        def body(i, _):
            o = pl.multiple_of(i * 128, 128)
            y_part[l, pl.ds(o, 128), cl] = dot(w_out_v[l, :, pl.ds(o, 128)], joined[:, cl], TN).astype(BF)
            return 0

        lax.fori_loop(0, width // 128, body, 0)
        for n, slot in enumerate((dd + flip, dx + flip, dy + flip, me + flip)):
            k = slot // 2
            cp = rcopy(y_part.at[l, pl.ds(slot * shard, shard), cl], d2d.at[l, k, :, cl],
                       d_ss.at[l, c, n], d_rs.at[l, c, n], dp_)
            cp.start()
            sends.append(cp)

    def chip_sum(l, c, slot, n, h=None, wait=True):
        k = slot // 2
        cl = pl.ds(c * cw, cw)
        if wait:
            ref = d2d.at[l, k, :, cl]
            rcopy(ref, ref, d_ss.at[l, c, n], d_rs.at[l, c, n], dp_).wait_recv()
        ln = cl if h is None else lanes(c, h)
        mine = y_part[l, pl.ds(pl.multiple_of(slot * shard, 16), shard), ln].astype(F32)
        return mine + d2d[l, k, :, ln].astype(F32)

    def rs_push(l, c, idx, value, dev):
        rs_send[l, c, idx] = value.astype(BF)
        cp = rcopy(rs_send.at[l, c, idx], rs_recv.at[l, c, idx], t_ss.at[l, c, idx], t_rs.at[l, c, idx], dev)
        cp.start()
        sends.append(cp)

    def rs_get(l, c, idx):
        ref = rs_recv.at[l, c, idx]
        rcopy(ref, ref, t_ss.at[l, c, idx], t_rs.at[l, c, idx], dp_).wait_recv()
        return rs_recv[l, c, idx].astype(F32)

    def rs_first(l, c):
        rs_push(l, c, 0, chip_sum(l, c, dd, 0, 0), dx)
        rs_push(l, c, 1, chip_sum(l, c, dd, 0, 1, wait=False), dy)
        rs_push(l, c, 2, chip_sum(l, c, dx, 1, 0), dx)
        rs_push(l, c, 5, chip_sum(l, c, dy, 2, 1), dy)

    def rs_second(l, c):
        rs_push(l, c, 4, chip_sum(l, c, dy, 2, 0, wait=False) + rs_get(l, c, 0), dy)
        rs_push(l, c, 3, chip_sum(l, c, dx, 1, 1, wait=False) + rs_get(l, c, 1), dx)

    def rs_last(l, c):
        first = chip_sum(l, c, me, 3, 0)
        second = chip_sum(l, c, me, 3, 1, wait=False)
        first = first + rs_get(l, c, 2) + rs_get(l, c, 4)
        second = second + rs_get(l, c, 5) + rs_get(l, c, 3)
        a, b = lanes(c, 0), lanes(c, 1)
        return ((r_all[l, me, :, a].astype(F32) + first).astype(BF),
                (r_all[l, me, :, b].astype(F32) + second).astype(BF))

    def keep(l, c, parts):
        r_all[l, me, :, lanes(c, 0)] = parts[0]
        r_all[l, me, :, lanes(c, 1)] = parts[1]
        ag_start(l, c)

    ln_start()
    ag_start(0, 0)
    ag_start(0, 1)
    setup_angles()
    ag_forward(0, 0)
    ag_relay(0, 0)
    ag_forward(0, 1)
    ln_finish()
    ag_finish(0, 0)
    ag_relay(0, 1)
    for l in range(layers):
        loads[("in", l)].wait()
        norm_query(l, 0)
        ag_finish(l, 1)
        loads[("key", l)].wait()
        loads[("val", l)].wait()
        norm_query(l, 1)
        key_value(l, 0)
        key_value(l, 1)
        feed_forward(l, 0)
        if l + 1 < layers:
            load_weights(l + 1)
        attention(l, 0)
        if l + 1 < layers:
            load_cache(l + 1, 0)
        feed_forward(l, 1)
        loads[("out", l)].wait()
        project(l, 0)
        attention(l, 1)
        if l + 1 < layers:
            load_cache(l + 1, 1)
        rs_first(l, 0)
        project(l, 1)
        rs_second(l, 0)
        rs_first(l, 1)
        parts = rs_last(l, 0)
        if l + 1 < layers:
            keep(l + 1, 0, parts)
            rs_second(l, 1)
            ag_forward(l + 1, 0)
            keep(l + 1, 1, rs_last(l, 1))
            ag_relay(l + 1, 0)
            ag_forward(l + 1, 1)
            ag_finish(l + 1, 0)
            ag_relay(l + 1, 1)
        else:
            rs_second(l, 1)
            full = jnp.concatenate(parts + rs_last(l, 1), axis=1)
            r_out[...] = dot(full, perm[...], NT).astype(BF)
    for cp in sends:
        cp.wait_send()


def cache_kernel(lengths, new_k, new_v, k_cache, v_cache, k_out, v_out, ring, in_sems, out_sems):
    layers, rows = k_cache.shape[:2]
    depth, per = ring.shape[0], ring.shape[1]
    groups = rows // per
    jobs = []
    for l in range(layers):
        for g in range(groups):
            jobs.append((k_cache, k_out, new_k, l, g))
            jobs.append((v_cache, v_out, new_v, l, g))
    n = len(jobs)
    ahead = depth - 6

    def fetch(i):
        src, _, _, l, g = jobs[i]
        return pltpu.make_async_copy(src.at[l, pl.ds(g * per, per)], ring.at[i % depth], in_sems.at[i % depth])

    def put(i):
        _, dst, _, l, g = jobs[i]
        return pltpu.make_async_copy(ring.at[i % depth], dst.at[l, pl.ds(g * per, per)], out_sems.at[i % depth])

    for i in range(ahead):
        fetch(i).start()
    for i in range(n):
        fetch(i).wait()
        _, _, new, l, g = jobs[i]
        fresh = new[l, pl.ds(g * per, per)]
        for b in range(per):
            slot = lengths[g * per + b]
            base = pl.multiple_of((slot // 16) * 16, 16)
            old = ring[i % depth, b, pl.ds(base, 16)].astype(F32)
            hit = iota2(old.shape, 0) == slot - base
            ring[i % depth, b, pl.ds(base, 16)] = jnp.where(hit, fresh[b:b + 1], old).astype(BF)
        put(i).start()
        nxt = i + ahead
        if nxt < n:
            if nxt >= depth:
                put(nxt - depth).wait()
            fetch(nxt).start()
    for i in range(max(0, n - depth), n):
        put(i).wait()


def solution(mesh):
    tp = mesh.shape["tp"]

    def device_step(residual, lengths, ln_scale, w_in, w_key, w_val, w_out, key_cache, val_cache):
        layers, width, in_cols = w_in.shape
        batch, shard = residual.shape
        rows = lengths.shape[0]
        head_dim = w_key.shape[2]
        ffn_dev = in_cols - w_out.shape[1]
        q_dev = w_out.shape[1] - ffn_dev
        heads = q_dev * tp // head_dim
        cw, cr = batch // CHUNKS, rows // CHUNKS
        hr = cr * heads
        slots = key_cache.shape[2]
        inv_freq = jnp.asarray((10000.0 ** (-np.arange(head_dim // 2) * (2.0 / head_dim))).astype(np.float32))[None, :]
        vmem = pl.BlockSpec(memory_space=pltpu.VMEM)
        hbm = pl.BlockSpec(memory_space=pltpu.HBM)
        smem = pl.BlockSpec(memory_space=pltpu.SMEM)
        dma = pltpu.SemaphoreType.DMA
        r_new, new_k, new_v = pl.pallas_call(
            step_kernel,
            out_shape=[jax.ShapeDtypeStruct((shard, batch), BF),
                       jax.ShapeDtypeStruct((layers, rows, head_dim), F32),
                       jax.ShapeDtypeStruct((layers, rows, head_dim), F32)],
            in_specs=[vmem] * 4 + [hbm] * 6,
            out_specs=[vmem] * 3,
            scratch_shapes=[
                pltpu.VMEM((layers, in_cols, width), BF),
                pltpu.VMEM((layers, width, head_dim), BF),
                pltpu.VMEM((layers, width, head_dim), BF),
                pltpu.VMEM((layers, w_out.shape[1], width), BF),
                pltpu.VMEM((rows, slots, head_dim), BF),
                pltpu.VMEM((rows, slots, head_dim), BF),
                pltpu.VMEM((layers, tp, shard, batch), BF),
                pltpu.VMEM((tp, layers, shard), BF),
                pltpu.VMEM((layers, tp, shard, 128), F32),
                pltpu.VMEM((width, batch), BF),
                pltpu.VMEM((ffn_dev + q_dev, batch), BF),
                pltpu.VMEM((layers, width, batch), BF),
                pltpu.VMEM((layers, tp // 2, shard, batch), BF),
                pltpu.VMEM((layers, CHUNKS, 6, shard, cw // 2), BF),
                pltpu.VMEM((layers, CHUNKS, 6, shard, cw // 2), BF),
                pltpu.VMEM((layers, batch, q_dev), BF),
                pltpu.VMEM((layers, CHUNKS, tp, cr, q_dev), BF),
                pltpu.VMEM((layers, CHUNKS, tp, cr, q_dev), BF),
                pltpu.VMEM((layers, CHUNKS, tp, cr, q_dev), BF),
                pltpu.VMEM((hr, head_dim), BF),
                pltpu.VMEM((hr, slots), F32),
                pltpu.VMEM((hr, head_dim), F32),
                pltpu.VMEM((128, head_dim), F32),
                pltpu.VMEM((CHUNKS, cr, head_dim // 2), F32),
                pltpu.VMEM((CHUNKS, cr, head_dim // 2), F32),
                pltpu.VMEM((CHUNKS, cr, 1), F32),
                pltpu.VMEM((CHUNKS, hr, 1), F32),
                pltpu.VMEM((batch, batch), BF),
                dma((layers, 4)), dma((layers, CHUNKS, 2)),
                dma((tp - 1,)), dma((tp - 1,)),
                dma((layers, CHUNKS, 14)), dma((layers, CHUNKS, tp, 2)),
                dma((layers, CHUNKS, tp - 1)), dma((layers, CHUNKS, tp - 1)),
                dma((layers, CHUNKS, tp - 1)), dma((layers, CHUNKS, tp - 1)),
                dma((layers, CHUNKS, 4)), dma((layers, CHUNKS, 4)),
                dma((layers, CHUNKS, 6)), dma((layers, CHUNKS, 6)),
            ],
            compiler_params=pltpu.CompilerParams(collective_id=0, has_side_effects=True, vmem_limit_bytes=60 * 2 ** 20),
            name="step",
        )(residual.T, lengths[None, :], ln_scale, inv_freq, jnp.swapaxes(w_in, 1, 2), w_key, w_val, w_out, key_cache, val_cache)
        key_out, val_out = pl.pallas_call(
            cache_kernel,
            out_shape=[jax.ShapeDtypeStruct(key_cache.shape, BF)] * 2,
            in_specs=[smem, vmem, vmem, hbm, hbm],
            out_specs=[hbm, hbm],
            scratch_shapes=[pltpu.VMEM((20, 8, slots, head_dim), BF), dma((20,)), dma((20,))],
            compiler_params=pltpu.CompilerParams(vmem_limit_bytes=40 * 2 ** 20),
            name="caches",
        )(lengths, new_k, new_v, key_cache, val_cache)
        return r_new.T, key_out, val_out

    cache_spec = P(None, ("dp", "tp"), None, None)
    return jax.shard_map(device_step, mesh=mesh, in_specs=(P("dp", "tp"), P(("dp", "tp")), P(None, "tp"), P(None, None, "tp"), P(), P(), P(None, "tp", None), cache_spec, cache_spec), out_specs=(P("dp", "tp"), cache_spec, cache_spec), check_vma=False)
```

```python
import functools

import jax
import jax.numpy as jnp
import numpy as np
from jax import lax
from jax.experimental import pallas as pl
from jax.experimental.pallas import tpu as pltpu
from jax.sharding import PartitionSpec as P

NORM_EPS = 1e-6
MESH = pl.DeviceIdType.MESH
CHUNKS = 2
BF = jnp.bfloat16
F32 = jnp.float32
TN = (((0,), (0,)), ((), ()))
NT = (((1,), (1,)), ((), ()))


def dot(a, b, dims=None):
    if dims is None:
        return jnp.dot(a, b, preferred_element_type=F32)
    return lax.dot_general(a, b, dims, preferred_element_type=F32)


def iota2(shape, dim):
    return lax.broadcasted_iota(jnp.int32, shape, dim)


def step_kernel(r_in, len_row, ln_in, inv_freq, w_in, w_key, w_val, w_out, k_cache, v_cache,
                r_out, new_k, new_v, kv_all,
                w_in_v, w_key_v, w_val_v, w_out_v, w_out_t,
                r_all, ln_all, ln_col, h_t, joined, y_part, d2d, rs_recv, rs_send,
                q_send, q_recv, o_send, o_recv, q_rows, s_rows, o_rows, kv_tmp,
                cos_b, sin_b, len_col, len_rep, perm,
                w_sems, c_sems, ln_ss, ln_rs, ag_ss, ag_rs, q_ss, q_rs, o_ss, o_rs, d_ss, d_rs, t_ss, t_rs):
    layers, width = w_in.shape[0], w_in.shape[2]
    shard, batch = r_in.shape
    tp = width // shard
    rows = batch // tp
    q_dev = q_send.shape[2]
    ffn_dev = w_out.shape[1] - q_dev
    head_dim = w_key.shape[2]
    half = head_dim // 2
    heads = q_dev * tp // head_dim
    cw = batch // CHUNKS
    cr = rows // CHUNKS
    hr = cr * heads

    me = lax.axis_index("tp")
    core, xpos, ypos = me % 2, (me // 2) % 2, me // 4
    dp_ = me + 1 - 2 * core
    dx = me + 2 - 4 * xpos
    dy = me + 4 - 8 * ypos
    dd = dx + 4 - 8 * ypos
    flip = 1 - 2 * core

    def rcopy(src, dst, ss, rs, dev):
        return pltpu.make_async_remote_copy(src_ref=src, dst_ref=dst, send_sem=ss, recv_sem=rs,
                                            device_id={"tp": dev}, device_id_type=MESH)

    barrier = pltpu.get_barrier_semaphore()
    for off in range(1, tp):
        pl.semaphore_signal(barrier, 1, device_id={"tp": (me + off) % tp}, device_id_type=MESH)

    loads = {}

    def load(name, src, dst, sem):
        loads[name] = pltpu.make_async_copy(src, dst, sem)
        loads[name].start()

    def load_in(l):
        load(("key", l), w_key.at[l], w_key_v, w_sems.at[l, 1])
        load(("val", l), w_val.at[l], w_val_v, w_sems.at[l, 2])
        load(("in", l), w_in.at[l], w_in_v, w_sems.at[l, 0])

    def load_out(l):
        load(("out", l), w_out.at[l], w_out_v, w_sems.at[l, 3])

    def load_cache(l):
        load(("k", l), k_cache.at[l], kv_all.at[0, l], c_sems.at[l, 0])
        load(("v", l), v_cache.at[l], kv_all.at[1, l], c_sems.at[l, 1])

    load_out(0)
    load_in(0)
    load_cache(0)

    src_i = iota2((batch, batch), 0)
    dst_i = iota2((batch, batch), 1)
    want = ((dst_i % cw) // cr) * rows + (dst_i // cw) * cr + dst_i % cr
    perm[...] = jnp.where(src_i == want, 1.0, 0.0).astype(BF)
    r_all[0, me] = dot(r_in[...], perm[...]).astype(BF)
    ln_all[me] = ln_in[...]

    pl.semaphore_wait(barrier, tp - 1)

    sends = []

    def lanes(c):
        return pl.ds(c * cw, cw)

    def ag_send(l, c, idx, dev, slot):
        ref = r_all.at[l, slot, :, lanes(c)]
        cp = rcopy(ref, ref, ag_ss.at[l, c, idx], ag_rs.at[l, c, slot], dev)
        cp.start()
        sends.append(cp)

    def ag_wait(l, c, slot):
        ref = r_all.at[l, slot, :, lanes(c)]
        rcopy(ref, ref, ag_ss.at[l, c, 0], ag_rs.at[l, c, slot], dp_).wait_recv()

    def ag_start(l, c):
        ag_send(l, c, 0, dd, me)
        ag_send(l, c, 1, dx, me)
        ag_send(l, c, 2, dy, me)
        ag_send(l, c, 3, dp_, me)

    def ag_relay(l, c):
        for n, slot in enumerate((dx, dy, dd)):
            ag_wait(l, c, slot)
            ag_send(l, c, 4 + n, dp_, slot)

    def ag_finish(l, c):
        for slot in (dp_, dx + flip, dy + flip, dd + flip):
            ag_wait(l, c, slot)

    def ln_start():
        for off in range(1, tp):
            cp = rcopy(ln_all.at[me], ln_all.at[me], ln_ss.at[off - 1], ln_rs.at[off - 1], (me + off) % tp)
            cp.start()
            sends.append(cp)

    def ln_finish():
        for off in range(1, tp):
            ref = ln_all.at[(me + tp - off) % tp]
            rcopy(ref, ref, ln_ss.at[off - 1], ln_rs.at[off - 1], dp_).wait_recv()
        for l in range(layers):
            pick = jnp.where(iota2((layers, 128), 0) == l, 1.0, 0.0).astype(BF)
            for s in range(tp):
                ln_col[l, s] = dot(ln_all[s], pick, TN)

    def setup_angles():
        lens = len_row[...].astype(F32)
        for c in range(CHUNKS):
            own = iota2((cr, rows), 1) == iota2((cr, rows), 0) + c * cr
            lc = jnp.sum(jnp.where(own, lens, 0.0), axis=1, keepdims=True)
            len_col[c] = lc
            rep = iota2((hr, rows), 1) == iota2((hr, rows), 0) // heads + c * cr
            len_rep[c] = jnp.sum(jnp.where(rep, lens, 0.0), axis=1, keepdims=True)
            ang = lc * inv_freq[...]
            cos_b[c] = jnp.cos(ang)
            sin_b[c] = jnp.sin(ang)

    def norm_query(l, c):
        cl = pl.ds(c * cw, cw)
        total = jnp.zeros((shard, cw), F32)
        squares = jnp.zeros((shard, cw), F32)
        for s in range(tp):
            v = r_all[l, s, :, cl].astype(F32)
            total = total + v
            squares = squares + v * v
        mean = jnp.sum(total, axis=0, keepdims=True) / width
        var = jnp.sum(squares, axis=0, keepdims=True) / width - mean * mean
        inv = lax.rsqrt(var + NORM_EPS)
        for s in range(tp):
            v = r_all[l, s, :, cl].astype(F32)
            scale = ln_col[l, s]
            scale = jnp.concatenate([scale] * (cw // 128), axis=1)
            h_t[pl.ds(s * shard, shard), cl] = ((v - mean) * inv * scale).astype(BF)
        q_t = dot(w_in_v[pl.ds(2 * ffn_dev, q_dev), :], h_t[:, cl])
        q_send[l, cl] = jnp.transpose(q_t).astype(BF)
        for off in range(1, tp):
            dev = (me + off) % tp
            cp = rcopy(q_send.at[l, pl.ds(c * cw + dev * cr, cr)], q_recv.at[l, c, me],
                       q_ss.at[l, c, off - 1], q_rs.at[l, c, off - 1], dev)
            cp.start()
            sends.append(cp)
        q_recv[l, c, me] = q_send[l, pl.ds(pl.multiple_of(c * cw + me * cr, cr), cr)]

    def key_value(l, c):
        per = 128 // cr
        blk = h_t[:, pl.ds(pl.multiple_of(c * cw + (me // per) * 128, 128), 128)]
        here = pl.ds(pl.multiple_of((me % per) * cr, cr), cr)
        kv_tmp[...] = dot(blk, w_key_v[...], TN)
        k = kv_tmp[here].astype(BF).astype(F32)
        x1, x2 = k[:, :half], k[:, half:]
        co, si = cos_b[c], sin_b[c]
        new_k[l, pl.ds(c * cr, cr), :half] = (x1 * co - x2 * si).astype(BF).astype(F32)
        new_k[l, pl.ds(c * cr, cr), half:] = (x2 * co + x1 * si).astype(BF).astype(F32)
        kv_tmp[...] = dot(blk, w_val_v[...], TN)
        new_v[l, pl.ds(c * cr, cr)] = kv_tmp[here].astype(BF).astype(F32)

    def feed_forward(l, c):
        cl = pl.ds(c * cw, cw)
        tile = 288

        def body(i, _):
            o = pl.multiple_of(i * tile, 32)
            gate = dot(w_in_v[pl.ds(o, tile)], h_t[:, cl]).astype(BF).astype(F32)
            up = dot(w_in_v[pl.ds(o + ffn_dev, tile)], h_t[:, cl]).astype(BF).astype(F32)
            joined[pl.ds(o, tile), cl] = (gate * jax.nn.sigmoid(gate) * up).astype(BF)
            return 0

        lax.fori_loop(0, ffn_dev // tile, body, 0)

    def attention(l, c):
        for off in range(1, tp):
            ref = q_recv.at[l, c, (me + tp - off) % tp]
            rcopy(ref, ref, q_ss.at[l, c, off - 1], q_rs.at[l, c, off - 1], dp_).wait_recv()
        co, si = cos_b[c], sin_b[c]
        r1, r2 = [], []
        for h in range(heads):
            x1 = q_recv[l, c, 2 * h].astype(F32)
            x2 = q_recv[l, c, 2 * h + 1].astype(F32)
            r1.append((x1 * co - x2 * si).astype(BF))
            r2.append((x2 * co + x1 * si).astype(BF))
        ri, ci = iota2((hr, hr), 0), iota2((hr, hr), 1)
        mix = jnp.where(ci == (ri % heads) * cr + ri // heads, 1.0, 0.0).astype(BF)
        q_rows[:, :half] = dot(mix, jnp.concatenate(r1, axis=0)).astype(BF)
        q_rows[:, half:] = dot(mix, jnp.concatenate(r2, axis=0)).astype(BF)
        rep = jnp.where(iota2((hr, cr), 1) == iota2((hr, cr), 0) // heads, 1.0, 0.0).astype(BF)
        k_rep = dot(rep, new_k[l, pl.ds(c * cr, cr)].astype(BF))
        v_rep = dot(rep, new_v[l, pl.ds(c * cr, cr)].astype(BF))
        q_all = q_rows[...].astype(F32)
        s_new = jnp.sum(q_all * k_rep, axis=1, keepdims=True) * head_dim ** -0.5
        group = 16 // heads
        which = iota2((16, head_dim), 0) // heads
        if c == 0:
            loads[("k", l)].wait()

        def score(g, _):
            o = pl.multiple_of(g * 16, 16)
            qg = q_rows[pl.ds(o, 16)]
            acc = jnp.zeros((16, head_dim), F32)
            for j in range(group):
                acc = jnp.where(which == j, dot(qg, kv_all[0, l, c * cr + g * group + j], NT), acc)
            s_rows[pl.ds(o, 16)] = acc
            return 0

        lax.fori_loop(0, hr // 16, score, 0, unroll=4)
        s = s_rows[...] * head_dim ** -0.5
        pos = iota2((hr, s.shape[1]), 1).astype(F32)
        s = jnp.where(pos < len_rep[c], s, -1e30)
        top = jnp.maximum(jnp.max(s, axis=1, keepdims=True), s_new)
        w = jnp.exp(s - top)
        w_new = jnp.exp(s_new - top)
        total = jnp.sum(w, axis=1, keepdims=True) + w_new
        q_rows[...] = w.astype(BF)
        if c == 0:
            loads[("v", l)].wait()

        def mixv(g, _):
            o = pl.multiple_of(g * 16, 16)
            wg = q_rows[pl.ds(o, 16)]
            acc = jnp.zeros((16, head_dim), F32)
            for j in range(group):
                acc = jnp.where(which == j, dot(wg, kv_all[1, l, c * cr + g * group + j]), acc)
            o_rows[pl.ds(o, 16)] = acc
            return 0

        lax.fori_loop(0, hr // 16, mixv, 0, unroll=4)
        mixed = (o_rows[...] + w_new.astype(BF).astype(F32) * v_rep) / total
        back = jnp.where(ri == (ci % heads) * cr + ci // heads, 1.0, 0.0).astype(BF)
        heads_o = dot(back, mixed.astype(BF)).astype(BF)
        for t in range(tp):
            o_send[l, c, t] = heads_o[(t // 2) * cr:(t // 2 + 1) * cr, (t % 2) * half:(t % 2 + 1) * half]
        for off in range(1, tp):
            dev = (me + off) % tp
            cp = rcopy(o_send.at[l, c, dev], o_recv.at[l, c, me], o_ss.at[l, c, off - 1], o_rs.at[l, c, off - 1], dev)
            cp.start()
            sends.append(cp)
        o_recv[l, c, me] = o_send[l, c, me]

    def project(l, c):
        cl = pl.ds(c * cw, cw)
        for off in range(1, tp):
            ref = o_recv.at[l, c, (me + tp - off) % tp]
            rcopy(ref, ref, o_ss.at[l, c, off - 1], o_rs.at[l, c, off - 1], dp_).wait_recv()
        o_all = jnp.concatenate([o_recv[l, c, j].astype(F32) for j in range(tp)], axis=0)
        joined[pl.ds(ffn_dev, q_dev), cl] = jnp.transpose(o_all).astype(BF)

        for n, slot in enumerate((dd + flip, dx + flip, dy + flip, me + flip, dd, dx, dy, me)):
            at = pl.ds(pl.multiple_of(slot * shard, 16), shard)
            y_part[l, at, cl] = dot(w_out_t[at], joined[:, cl]).astype(BF)
            if n < 4:
                cp = rcopy(y_part.at[l, at, cl], d2d.at[l, slot // 2, :, cl], d_ss.at[l, c, n], d_rs.at[l, c, n], dp_)
                cp.start()
                sends.append(cp)

    def turn_out(l):
        loads[("out", l)].wait()

        def body(i, _):
            o = pl.multiple_of(i * 128, 128)
            w_out_t[pl.ds(o, 128)] = jnp.transpose(w_out_v[:, pl.ds(o, 128)])
            return 0

        lax.fori_loop(0, width // 128, body, 0)

    def chip_sum(l, c, slot, n):
        ref = d2d.at[l, slot // 2, :, lanes(c)]
        rcopy(ref, ref, d_ss.at[l, c, n], d_rs.at[l, c, n], dp_).wait_recv()
        mine = y_part[l, pl.ds(pl.multiple_of(slot * shard, 16), shard), lanes(c)].astype(F32)
        return mine + d2d[l, slot // 2, :, lanes(c)].astype(F32)

    def rs_first(l, c):
        for n, dev in enumerate((dd, dx, dy)):
            rs_send[l, c, n] = chip_sum(l, c, dev, n).astype(BF)
            cp = rcopy(rs_send.at[l, c, n], rs_recv.at[l, c, n], t_ss.at[l, c, n], t_rs.at[l, c, n], dev)
            cp.start()
            sends.append(cp)

    def rs_last(l, c):
        total = chip_sum(l, c, me, 3)
        for n in (1, 2, 0):
            ref = rs_recv.at[l, c, n]
            rcopy(ref, ref, t_ss.at[l, c, n], t_rs.at[l, c, n], dp_).wait_recv()
            total = total + rs_recv[l, c, n].astype(F32)
        return (r_all[l, me, :, lanes(c)].astype(F32) + total).astype(BF)

    def keep(l, c, part):
        r_all[l, me, :, lanes(c)] = part
        ag_start(l, c)

    ln_start()
    ag_start(0, 0)
    ag_start(0, 1)
    setup_angles()
    turn_out(0)
    ag_relay(0, 0)
    ln_finish()
    ag_finish(0, 0)
    for l in range(layers):
        loads[("in", l)].wait()
        norm_query(l, 0)
        load_cache(l + 1) if l + 1 < layers else None
        ag_relay(l, 1)
        ag_finish(l, 1)
        norm_query(l, 1)
        loads[("key", l)].wait()
        loads[("val", l)].wait()
        key_value(l, 0)
        key_value(l, 1)
        feed_forward(l, 0)
        attention(l, 0)
        attention(l, 1)
        feed_forward(l, 1)
        if l + 1 < layers:
            load_in(l + 1)
            load_out(l + 1)
        project(l, 0)
        project(l, 1)
        rs_first(l, 0)
        rs_first(l, 1)
        if l + 1 < layers:
            turn_out(l + 1)
            keep(l + 1, 0, rs_last(l, 0))
            keep(l + 1, 1, rs_last(l, 1))
            ag_relay(l + 1, 0)
            ag_finish(l + 1, 0)
        else:
            full = jnp.concatenate([rs_last(l, 0), rs_last(l, 1)], axis=1)
            r_out[...] = dot(full, perm[...], NT).astype(BF)
    for cp in sends:
        cp.wait_send()


def cache_kernel(lengths, new_k, new_v, kv_all, k_out, v_out, tiles, big_sems, tile_sems):
    layers, rows = kv_all.shape[1:3]
    per = 16
    pairs = [(kv_all.at[0], k_out, new_k, 0), (kv_all.at[1], v_out, new_v, 1)]
    jobs = [(l, g, pair) for l in range(layers) for pair in pairs for g in range(rows // per)]

    def big(i):
        l, g, (src, dst, _, _) = jobs[i]
        at = pl.ds(g * per, per)
        return pltpu.make_async_copy(src.at[l, at], dst.at[l, at], big_sems.at[i])

    for i in range(len(jobs)):
        big(i).start()

    def build(b, _):
        slot = lengths[b]
        base = pl.multiple_of((slot // 16) * 16, 16)
        hit = iota2((16, kv_all.shape[4]), 0) == slot - base
        for l in range(layers):
            for src, _, new, n in pairs:
                old = src[l, b, pl.ds(base, 16)].astype(F32)
                tiles[l, n, b] = jnp.where(hit, new[l, pl.ds(b, 1)], old).astype(BF)
        return 0

    lax.fori_loop(0, rows, build, 0, unroll=4)
    for i in range(len(jobs)):
        l, g, (_, dst, _, n) = jobs[i]
        big(i).wait()

        def patch(j, _):
            b = g * per + j
            base = pl.multiple_of((lengths[b] // 16) * 16, 16)
            pltpu.make_async_copy(tiles.at[l, n, b], dst.at[l, b, pl.ds(base, 16)], tile_sems.at[i]).start()
            return 0

        lax.fori_loop(0, per, patch, 0, unroll=4)
    for i in range(len(jobs)):
        l, g, (_, dst, _, n) = jobs[i]
        at = pl.ds(g * per, per)
        pltpu.make_async_copy(tiles.at[l, n, at], dst.at[l, at, pl.ds(0, 16)], tile_sems.at[i]).wait()


def solution(mesh):
    tp = mesh.shape["tp"]

    def device_step(residual, lengths, ln_scale, w_in, w_key, w_val, w_out, key_cache, val_cache):
        layers, width, in_cols = w_in.shape
        batch, shard = residual.shape
        rows = lengths.shape[0]
        head_dim = w_key.shape[2]
        ffn_dev = in_cols - w_out.shape[1]
        q_dev = w_out.shape[1] - ffn_dev
        heads = q_dev * tp // head_dim
        cw, cr = batch // CHUNKS, rows // CHUNKS
        hr = cr * heads
        slots = key_cache.shape[2]
        inv_freq = jnp.asarray((10000.0 ** (-np.arange(head_dim // 2) * (2.0 / head_dim))).astype(np.float32))[None, :]
        vmem = pl.BlockSpec(memory_space=pltpu.VMEM)
        hbm = pl.BlockSpec(memory_space=pltpu.HBM)
        smem = pl.BlockSpec(memory_space=pltpu.SMEM)
        dma = pltpu.SemaphoreType.DMA
        r_new, new_k, new_v, kv_all = pl.pallas_call(
            step_kernel,
            out_shape=[jax.ShapeDtypeStruct((shard, batch), BF),
                       pltpu.VMEM((layers, rows, head_dim), F32),
                       pltpu.VMEM((layers, rows, head_dim), F32),
                       pltpu.VMEM((2,) + key_cache.shape, BF)],
            in_specs=[vmem] * 4 + [hbm] * 6,
            out_specs=[vmem] * 4,
            scratch_shapes=[
                pltpu.VMEM((in_cols, width), BF),
                pltpu.VMEM((width, head_dim), BF),
                pltpu.VMEM((width, head_dim), BF),
                pltpu.VMEM((w_out.shape[1], width), BF),
                pltpu.VMEM((width, w_out.shape[1]), BF),
                pltpu.VMEM((layers, tp, shard, batch), BF),
                pltpu.VMEM((tp, layers, shard), BF),
                pltpu.VMEM((layers, tp, shard, 128), F32),
                pltpu.VMEM((width, batch), BF),
                pltpu.VMEM((ffn_dev + q_dev, batch), BF),
                pltpu.VMEM((layers, width, batch), BF),
                pltpu.VMEM((layers, tp // 2, shard, batch), BF),
                pltpu.VMEM((layers, CHUNKS, 3, shard, cw), BF),
                pltpu.VMEM((layers, CHUNKS, 3, shard, cw), BF),
                pltpu.VMEM((layers, batch, q_dev), BF),
                pltpu.VMEM((layers, CHUNKS, tp, cr, q_dev), BF),
                pltpu.VMEM((layers, CHUNKS, tp, cr, q_dev), BF),
                pltpu.VMEM((layers, CHUNKS, tp, cr, q_dev), BF),
                pltpu.VMEM((hr, head_dim), BF),
                pltpu.VMEM((hr, slots), F32),
                pltpu.VMEM((hr, head_dim), F32),
                pltpu.VMEM((128, head_dim), F32),
                pltpu.VMEM((CHUNKS, cr, head_dim // 2), F32),
                pltpu.VMEM((CHUNKS, cr, head_dim // 2), F32),
                pltpu.VMEM((CHUNKS, cr, 1), F32),
                pltpu.VMEM((CHUNKS, hr, 1), F32),
                pltpu.VMEM((batch, batch), BF),
                dma((layers, 4)), dma((layers, 2)),
                dma((tp - 1,)), dma((tp - 1,)),
                dma((layers, CHUNKS, 7)), dma((layers, CHUNKS, tp)),
                dma((layers, CHUNKS, tp - 1)), dma((layers, CHUNKS, tp - 1)),
                dma((layers, CHUNKS, tp - 1)), dma((layers, CHUNKS, tp - 1)),
                dma((layers, CHUNKS, 4)), dma((layers, CHUNKS, 4)),
                dma((layers, CHUNKS, 3)), dma((layers, CHUNKS, 3)),
            ],
            compiler_params=pltpu.CompilerParams(collective_id=0, has_side_effects=True, vmem_limit_bytes=27 * 2 ** 20),
            name="step",
        )(residual.T, lengths[None, :], ln_scale, inv_freq, jnp.swapaxes(w_in, 1, 2), w_key, w_val, w_out, key_cache, val_cache)
        keep = functools.partial(pltpu.with_memory_space_constraint, memory_space=pltpu.VMEM)
        key_out, val_out = pl.pallas_call(
            cache_kernel,
            out_shape=[jax.ShapeDtypeStruct(key_cache.shape, BF)] * 2,
            in_specs=[smem] + [vmem] * 3,
            out_specs=[hbm, hbm],
            scratch_shapes=[pltpu.VMEM((layers, 2, rows, 16, head_dim), BF), dma((16,)), dma((16,))],
            compiler_params=pltpu.CompilerParams(vmem_limit_bytes=5 * 2 ** 20),
            name="caches",
        )(lengths, keep(new_k), keep(new_v), keep(kv_all))
        return r_new.T, key_out, val_out

    cache_spec = P(None, ("dp", "tp"), None, None)
    return jax.shard_map(device_step, mesh=mesh, in_specs=(P("dp", "tp"), P(("dp", "tp")), P(None, "tp"), P(None, None, "tp"), P(), P(), P(None, "tp", None), cache_spec, cache_spec), out_specs=(P("dp", "tp"), cache_spec, cache_spec), check_vma=False)
```

```python
import functools

import jax
import jax.numpy as jnp
import numpy as np
from jax import lax
from jax.experimental import pallas as pl
from jax.experimental.pallas import tpu as pltpu
from jax.sharding import PartitionSpec as P

NORM_EPS = 1e-6
MESH = pl.DeviceIdType.MESH
CHUNKS = 2
BF = jnp.bfloat16
F32 = jnp.float32
TN = (((0,), (0,)), ((), ()))
NT = (((1,), (1,)), ((), ()))


def dot(a, b, dims=None):
    if dims is None:
        return jnp.dot(a, b, preferred_element_type=F32)
    return lax.dot_general(a, b, dims, preferred_element_type=F32)


def iota2(shape, dim):
    return lax.broadcasted_iota(jnp.int32, shape, dim)


def step_kernel(r_in, len_row, ln_in, inv_freq, w_in, w_key, w_val, w_out, k_cache, v_cache,
                sum_d, sum_x, sum_y, base, new_k, new_v, kv_all,
                w_in_v, w_key_v, w_val_v, w_out_v, w_out_t,
                r_all, ln_all, ln_col, h_t, joined, y_part, d2d, rs_recv, rs_send,
                q_send, q_recv, o_send, o_recv, q_rows, s_rows, o_rows, kv_tmp,
                cos_b, sin_b, len_col, len_rep, perm, r_buf, r_sem,
                w_sems, c_sems, ln_ss, ln_rs, ag_ss, ag_rs, q_ss, q_rs, o_ss, o_rs, d_ss, d_rs, t_ss, t_rs):
    layers, width = w_in.shape[0], w_in.shape[2]
    shard, batch = r_in.shape
    tp = width // shard
    rows = batch // tp
    q_dev = q_send.shape[2]
    ffn_dev = w_out.shape[1] - q_dev
    head_dim = w_key.shape[2]
    half = head_dim // 2
    heads = q_dev * tp // head_dim
    cw = batch // CHUNKS
    cr = rows // CHUNKS
    hr = cr * heads

    me = lax.axis_index("tp")
    core, xpos, ypos = me % 2, (me // 2) % 2, me // 4
    dp_ = me + 1 - 2 * core
    dx = me + 2 - 4 * xpos
    dy = me + 4 - 8 * ypos
    dd = dx + 4 - 8 * ypos
    flip = 1 - 2 * core

    def rcopy(src, dst, ss, rs, dev):
        return pltpu.make_async_remote_copy(src_ref=src, dst_ref=dst, send_sem=ss, recv_sem=rs,
                                            device_id={"tp": dev}, device_id_type=MESH)

    barrier = pltpu.get_barrier_semaphore()
    for off in range(1, tp):
        pl.semaphore_signal(barrier, 1, device_id={"tp": (me + off) % tp}, device_id_type=MESH)

    r_load = pltpu.make_async_copy(r_in, r_buf, r_sem)
    r_load.start()

    loads = {}

    def load(name, src, dst, sem):
        loads[name] = pltpu.make_async_copy(src, dst, sem)
        loads[name].start()

    def load_in(l):
        load(("key", l), w_key.at[l], w_key_v, w_sems.at[l, 1])
        load(("val", l), w_val.at[l], w_val_v, w_sems.at[l, 2])
        load(("in", l), w_in.at[l], w_in_v, w_sems.at[l, 0])

    def load_out(l):
        load(("out", l), w_out.at[l], w_out_v, w_sems.at[l, 3])

    def load_cache(l):
        load(("k", l), k_cache.at[l], kv_all.at[0, l], c_sems.at[l, 0])
        load(("v", l), v_cache.at[l], kv_all.at[1, l], c_sems.at[l, 1])

    perm[...] = order(cw, cr, rows, batch)
    r_load.wait()
    load_out(0)
    load_in(0)
    r_all[0, me] = dot(r_buf[...], perm[...]).astype(BF)
    ln_all[me] = ln_in[...]

    pl.semaphore_wait(barrier, tp - 1)

    sends = []

    def lanes(c):
        return pl.ds(c * cw, cw)

    def ag_send(l, c, idx, dev, slot):
        ref = r_all.at[l, slot, :, lanes(c)]
        cp = rcopy(ref, ref, ag_ss.at[l, c, idx], ag_rs.at[l, c, slot], dev)
        cp.start()
        sends.append(cp)

    def ag_wait(l, c, slot):
        ref = r_all.at[l, slot, :, lanes(c)]
        rcopy(ref, ref, ag_ss.at[l, c, 0], ag_rs.at[l, c, slot], dp_).wait_recv()

    def ag_start(l, c):
        ag_send(l, c, 0, dd, me)
        ag_send(l, c, 1, dx, me)
        ag_send(l, c, 2, dy, me)
        ag_send(l, c, 3, dp_, me)

    def ag_relay(l, c):
        for n, slot in enumerate((dx, dy, dd)):
            ag_wait(l, c, slot)
            ag_send(l, c, 4 + n, dp_, slot)

    def ag_finish(l, c):
        for slot in (dp_, dx + flip, dy + flip, dd + flip):
            ag_wait(l, c, slot)

    def ln_start():
        for off in range(1, tp):
            cp = rcopy(ln_all.at[me], ln_all.at[me], ln_ss.at[off - 1], ln_rs.at[off - 1], (me + off) % tp)
            cp.start()
            sends.append(cp)

    def ln_finish():
        for off in range(1, tp):
            ref = ln_all.at[(me + tp - off) % tp]
            rcopy(ref, ref, ln_ss.at[off - 1], ln_rs.at[off - 1], dp_).wait_recv()
        for l in range(layers):
            pick = jnp.where(iota2((layers, 128), 0) == l, 1.0, 0.0).astype(BF)
            for s in range(tp):
                ln_col[l, s] = dot(ln_all[s], pick, TN)

    def setup_angles():
        lens = len_row[...].astype(F32)
        for c in range(CHUNKS):
            own = iota2((cr, rows), 1) == iota2((cr, rows), 0) + c * cr
            lc = jnp.sum(jnp.where(own, lens, 0.0), axis=1, keepdims=True)
            len_col[c] = lc
            rep = iota2((hr, rows), 1) == lax.shift_right_logical(iota2((hr, rows), 0), heads.bit_length() - 1) + c * cr
            len_rep[c] = jnp.sum(jnp.where(rep, lens, 0.0), axis=1, keepdims=True)
            ang = lc * inv_freq[...]
            cos_b[c] = jnp.cos(ang)
            sin_b[c] = jnp.sin(ang)

    def norm_query(l, c):
        cl = pl.ds(c * cw, cw)
        total = jnp.zeros((shard, cw), F32)
        squares = jnp.zeros((shard, cw), F32)
        for s in range(tp):
            v = r_all[l, s, :, cl].astype(F32)
            total = total + v
            squares = squares + v * v
        mean = jnp.sum(total, axis=0, keepdims=True) / width
        var = jnp.sum(squares, axis=0, keepdims=True) / width - mean * mean
        inv = lax.rsqrt(var + NORM_EPS)
        for s in range(tp):
            v = r_all[l, s, :, cl].astype(F32)
            scale = ln_col[l, s]
            scale = jnp.concatenate([scale] * (cw // 128), axis=1)
            h_t[pl.ds(s * shard, shard), cl] = ((v - mean) * inv * scale).astype(BF)
        q_t = dot(w_in_v[pl.ds(2 * ffn_dev, q_dev), :], h_t[:, cl])
        q_send[l, cl] = jnp.transpose(q_t).astype(BF)
        for off in range(1, tp):
            dev = (me + off) % tp
            cp = rcopy(q_send.at[l, pl.ds(c * cw + dev * cr, cr)], q_recv.at[l, c, me],
                       q_ss.at[l, c, off - 1], q_rs.at[l, c, off - 1], dev)
            cp.start()
            sends.append(cp)
        q_recv[l, c, me] = q_send[l, pl.ds(pl.multiple_of(c * cw + me * cr, cr), cr)]

    def key_value(l, c):
        per = 128 // cr
        blk = h_t[:, pl.ds(pl.multiple_of(c * cw + (me // per) * 128, 128), 128)]
        here = pl.ds(pl.multiple_of((me % per) * cr, cr), cr)
        kv_tmp[...] = dot(blk, w_key_v[...], TN)
        k = kv_tmp[here].astype(BF).astype(F32)
        x1, x2 = k[:, :half], k[:, half:]
        co, si = cos_b[c], sin_b[c]
        new_k[l, pl.ds(c * cr, cr), :half] = (x1 * co - x2 * si).astype(BF).astype(F32)
        new_k[l, pl.ds(c * cr, cr), half:] = (x2 * co + x1 * si).astype(BF).astype(F32)
        kv_tmp[...] = dot(blk, w_val_v[...], TN)
        new_v[l, pl.ds(c * cr, cr)] = kv_tmp[here].astype(BF).astype(F32)

    def feed_forward(l, c):
        cl = pl.ds(c * cw, cw)
        tile = 432

        def body(i, _):
            o = pl.multiple_of(i * tile, 16)
            gate = dot(w_in_v[pl.ds(o, tile)], h_t[:, cl]).astype(BF).astype(F32)
            up = dot(w_in_v[pl.ds(o + ffn_dev, tile)], h_t[:, cl]).astype(BF).astype(F32)
            joined[pl.ds(o, tile), cl] = (gate * jax.nn.sigmoid(gate) * up).astype(BF)
            return 0

        lax.fori_loop(0, ffn_dev // tile, body, 0)

    def attention(l, c):
        for off in range(1, tp):
            ref = q_recv.at[l, c, (me + tp - off) % tp]
            rcopy(ref, ref, q_ss.at[l, c, off - 1], q_rs.at[l, c, off - 1], dp_).wait_recv()
        co, si = cos_b[c], sin_b[c]
        r1, r2 = [], []
        for h in range(heads):
            x1 = q_recv[l, c, 2 * h].astype(F32)
            x2 = q_recv[l, c, 2 * h + 1].astype(F32)
            r1.append((x1 * co - x2 * si).astype(BF))
            r2.append((x2 * co + x1 * si).astype(BF))
        ri, ci = iota2((hr, hr), 0), iota2((hr, hr), 1)
        mix = jnp.where(ci == (ri & (heads - 1)) * cr + lax.shift_right_logical(ri, heads.bit_length() - 1), 1.0, 0.0).astype(BF)
        q_rows[:, :half] = dot(mix, jnp.concatenate(r1, axis=0)).astype(BF)
        q_rows[:, half:] = dot(mix, jnp.concatenate(r2, axis=0)).astype(BF)
        rep = jnp.where(iota2((hr, cr), 1) == lax.shift_right_logical(iota2((hr, cr), 0), heads.bit_length() - 1), 1.0, 0.0).astype(BF)
        k_rep = dot(rep, new_k[l, pl.ds(c * cr, cr)].astype(BF))
        v_rep = dot(rep, new_v[l, pl.ds(c * cr, cr)].astype(BF))
        q_all = q_rows[...].astype(F32)
        s_new = jnp.sum(q_all * k_rep, axis=1, keepdims=True) * head_dim ** -0.5
        group = 16 // heads
        which = lax.shift_right_logical(iota2((16, head_dim), 0), heads.bit_length() - 1)
        if c == 0:
            loads[("k", l)].wait()

        def score(g, _):
            o = pl.multiple_of(g * 16, 16)
            qg = q_rows[pl.ds(o, 16)]
            acc = jnp.zeros((16, head_dim), F32)
            for j in range(group):
                acc = jnp.where(which == j, dot(qg, kv_all[0, l, c * cr + g * group + j], NT), acc)
            s_rows[pl.ds(o, 16)] = acc
            return 0

        lax.fori_loop(0, hr // 16, score, 0, unroll=4)
        s = s_rows[...] * head_dim ** -0.5
        pos = iota2((hr, s.shape[1]), 1).astype(F32)
        s = jnp.where(pos < len_rep[c], s, -1e30)
        top = jnp.maximum(jnp.max(s, axis=1, keepdims=True), s_new)
        w = jnp.exp(s - top)
        w_new = jnp.exp(s_new - top)
        total = jnp.sum(w, axis=1, keepdims=True) + w_new
        q_rows[...] = w.astype(BF)
        if c == 0:
            loads[("v", l)].wait()

        def mixv(g, _):
            o = pl.multiple_of(g * 16, 16)
            wg = q_rows[pl.ds(o, 16)]
            acc = jnp.zeros((16, head_dim), F32)
            for j in range(group):
                acc = jnp.where(which == j, dot(wg, kv_all[1, l, c * cr + g * group + j]), acc)
            o_rows[pl.ds(o, 16)] = acc
            return 0

        lax.fori_loop(0, hr // 16, mixv, 0, unroll=4)
        mixed = (o_rows[...] + w_new.astype(BF).astype(F32) * v_rep) / total
        back = jnp.where(ri == (ci & (heads - 1)) * cr + lax.shift_right_logical(ci, heads.bit_length() - 1), 1.0, 0.0).astype(BF)
        heads_o = dot(back, mixed.astype(BF)).astype(BF)
        for t in range(tp):
            o_send[l, c, t] = heads_o[(t // 2) * cr:(t // 2 + 1) * cr, (t % 2) * half:(t % 2 + 1) * half]
        for off in range(1, tp):
            dev = (me + off) % tp
            cp = rcopy(o_send.at[l, c, dev], o_recv.at[l, c, me], o_ss.at[l, c, off - 1], o_rs.at[l, c, off - 1], dev)
            cp.start()
            sends.append(cp)
        o_recv[l, c, me] = o_send[l, c, me]

    def project(l, c):
        cl = pl.ds(c * cw, cw)
        for off in range(1, tp):
            ref = o_recv.at[l, c, (me + tp - off) % tp]
            rcopy(ref, ref, o_ss.at[l, c, off - 1], o_rs.at[l, c, off - 1], dp_).wait_recv()
        o_all = jnp.concatenate([o_recv[l, c, j].astype(F32) for j in range(tp)], axis=0)
        joined[pl.ds(ffn_dev, q_dev), cl] = jnp.transpose(o_all).astype(BF)

        for n, slot in enumerate((dd + flip, dx + flip, dy + flip, me + flip, dd, dx, dy, me)):
            at = pl.ds(pl.multiple_of(slot * shard, 16), shard)
            y_part[l, at, cl] = dot(w_out_t[at], joined[:, cl]).astype(BF)
            if n < 4:
                cp = rcopy(y_part.at[l, at, cl], d2d.at[l, slot // 2, :, cl], d_ss.at[l, c, n], d_rs.at[l, c, n], dp_)
                cp.start()
                sends.append(cp)

    def turn_out(l):
        loads[("out", l)].wait()

        def body(i, _):
            o = pl.multiple_of(i * 128, 128)
            w_out_t[pl.ds(o, 128)] = jnp.transpose(w_out_v[:, pl.ds(o, 128)])
            return 0

        lax.fori_loop(0, width // 128, body, 0)

    def chip_sum(l, c, slot, n):
        ref = d2d.at[l, slot // 2, :, lanes(c)]
        rcopy(ref, ref, d_ss.at[l, c, n], d_rs.at[l, c, n], dp_).wait_recv()
        mine = y_part[l, pl.ds(pl.multiple_of(slot * shard, 16), shard), lanes(c)].astype(F32)
        return mine + d2d[l, slot // 2, :, lanes(c)].astype(F32)

    def rs_first(l, c):
        for n, dev in enumerate((dd, dx, dy)):
            rs_send[l, c, n] = chip_sum(l, c, dev, n).astype(BF)
            cp = rcopy(rs_send.at[l, c, n], rs_recv.at[l, c, n], t_ss.at[l, c, n], t_rs.at[l, c, n], dev)
            cp.start()
            sends.append(cp)

    def chip_sums(l, c):
        for n, (out, dev) in enumerate(((sum_d, dd), (sum_x, dx), (sum_y, dy))):
            out[:, lanes(c)] = chip_sum(l, c, dev, n).astype(BF)
        base[:, lanes(c)] = r_all[l, me, :, lanes(c)].astype(F32) + chip_sum(l, c, me, 3)

    def rs_last(l, c):
        total = chip_sum(l, c, me, 3)
        for n in (1, 2, 0):
            ref = rs_recv.at[l, c, n]
            rcopy(ref, ref, t_ss.at[l, c, n], t_rs.at[l, c, n], dp_).wait_recv()
            total = total + rs_recv[l, c, n].astype(F32)
        return (r_all[l, me, :, lanes(c)].astype(F32) + total).astype(BF)

    def keep(l, c, part):
        r_all[l, me, :, lanes(c)] = part
        ag_start(l, c)

    ln_start()
    ag_start(0, 0)
    ag_start(0, 1)
    load_cache(0)
    setup_angles()
    turn_out(0)
    ag_relay(0, 0)
    ln_finish()
    ag_finish(0, 0)
    for l in range(layers):
        last = l + 1 == layers
        loads[("in", l)].wait()
        norm_query(l, 0)
        if not last:
            load_cache(l + 1)
        loads[("key", l)].wait()
        loads[("val", l)].wait()
        key_value(l, 0)
        if l == 0:
            ag_relay(l, 1)
            feed_forward(l, 0)
        else:
            feed_forward(l, 0)
            ag_relay(l, 1)
        ag_finish(l, 1)
        norm_query(l, 1)
        key_value(l, 1)
        attention(l, 0)
        feed_forward(l, 1)
        if not last:
            load_in(l + 1)
            load_out(l + 1)
        attention(l, 1)
        project(l, 0)
        if last:
            chip_sums(l, 0)
        else:
            rs_first(l, 0)
        project(l, 1)
        if last:
            chip_sums(l, 1)
        else:
            rs_first(l, 1)
            turn_out(l + 1)
            keep(l + 1, 0, rs_last(l, 0))
            keep(l + 1, 1, rs_last(l, 1))
            ag_relay(l + 1, 0)
            ag_finish(l + 1, 0)
    for cp in sends:
        cp.wait_send()


def order(cw, cr, rows, batch):
    pos = iota2((1, batch), 1)
    want = ((pos & (cw - 1)) // cr) * rows + (pos // cw) * cr + (pos & (cr - 1))
    return jnp.where(iota2((batch, batch), 0) == want, 1.0, 0.0).astype(BF)


def final_kernel(cw, cr, rows, base, part_d, part_x, part_y, out):
    total = base[...] + part_d[...].astype(F32) + part_x[...].astype(F32) + part_y[...].astype(F32)
    out[...] = dot(total.astype(BF), order(cw, cr, rows, base.shape[1]), NT).astype(BF)


def cache_kernel(lengths, new_k, new_v, kv_all, k_out, v_out, tiles, big_sems, tile_sems):
    layers, rows = kv_all.shape[1:3]
    per = 16
    pairs = [(kv_all.at[0], k_out, new_k, 0), (kv_all.at[1], v_out, new_v, 1)]
    jobs = [(l, g, pair) for l in range(layers) for pair in pairs for g in range(rows // per)]

    def big(i):
        l, g, (src, dst, _, _) = jobs[i]
        at = pl.ds(g * per, per)
        return pltpu.make_async_copy(src.at[l, at], dst.at[l, at], big_sems.at[i])

    for i in range(len(jobs)):
        big(i).start()

    def build(b, _):
        slot = lengths[b]
        base = pl.multiple_of((slot // 16) * 16, 16)
        hit = iota2((16, kv_all.shape[4]), 0) == slot - base
        for l in range(layers):
            for src, _, new, n in pairs:
                old = src[l, b, pl.ds(base, 16)].astype(F32)
                tiles[l, n, b] = jnp.where(hit, new[l, pl.ds(b, 1)], old).astype(BF)
        return 0

    lax.fori_loop(0, rows, build, 0, unroll=4)
    for i in range(len(jobs)):
        l, g, (_, dst, _, n) = jobs[i]
        big(i).wait()

        def patch(j, _):
            b = g * per + j
            base = pl.multiple_of((lengths[b] // 16) * 16, 16)
            pltpu.make_async_copy(tiles.at[l, n, b], dst.at[l, b, pl.ds(base, 16)], tile_sems.at[i]).start()
            return 0

        lax.fori_loop(0, per, patch, 0, unroll=4)
    for i in range(len(jobs)):
        l, g, (_, dst, _, n) = jobs[i]
        at = pl.ds(g * per, per)
        pltpu.make_async_copy(tiles.at[l, n, at], dst.at[l, at, pl.ds(0, 16)], tile_sems.at[i]).wait()


def solution(mesh):
    tp = mesh.shape["tp"]

    def device_step(residual, lengths, ln_scale, w_in, w_key, w_val, w_out, key_cache, val_cache):
        layers, width, in_cols = w_in.shape
        batch, shard = residual.shape
        rows = lengths.shape[0]
        head_dim = w_key.shape[2]
        ffn_dev = in_cols - w_out.shape[1]
        q_dev = w_out.shape[1] - ffn_dev
        heads = q_dev * tp // head_dim
        cw, cr = batch // CHUNKS, rows // CHUNKS
        hr = cr * heads
        slots = key_cache.shape[2]
        inv_freq = jnp.asarray((10000.0 ** (-np.arange(head_dim // 2) * (2.0 / head_dim))).astype(np.float32))[None, :]
        vmem = pl.BlockSpec(memory_space=pltpu.VMEM)
        hbm = pl.BlockSpec(memory_space=pltpu.HBM)
        smem = pl.BlockSpec(memory_space=pltpu.SMEM)
        dma = pltpu.SemaphoreType.DMA
        sum_d, sum_x, sum_y, base, new_k, new_v, kv_all = pl.pallas_call(
            step_kernel,
            out_shape=[pltpu.VMEM((shard, batch), BF)] * 3 + [
                       pltpu.VMEM((shard, batch), F32),
                       pltpu.VMEM((layers, rows, head_dim), F32),
                       pltpu.VMEM((layers, rows, head_dim), F32),
                       pltpu.VMEM((2,) + key_cache.shape, BF)],
            in_specs=[hbm] + [vmem] * 3 + [hbm] * 6,
            out_specs=[vmem] * 7,
            scratch_shapes=[
                pltpu.VMEM((in_cols, width), BF),
                pltpu.VMEM((width, head_dim), BF),
                pltpu.VMEM((width, head_dim), BF),
                pltpu.VMEM((w_out.shape[1], width), BF),
                pltpu.VMEM((width, w_out.shape[1]), BF),
                pltpu.VMEM((layers, tp, shard, batch), BF),
                pltpu.VMEM((tp, layers, shard), BF),
                pltpu.VMEM((layers, tp, shard, 128), F32),
                pltpu.VMEM((width, batch), BF),
                pltpu.VMEM((ffn_dev + q_dev, batch), BF),
                pltpu.VMEM((layers, width, batch), BF),
                pltpu.VMEM((layers, tp // 2, shard, batch), BF),
                pltpu.VMEM((layers, CHUNKS, 3, shard, cw), BF),
                pltpu.VMEM((layers, CHUNKS, 3, shard, cw), BF),
                pltpu.VMEM((layers, batch, q_dev), BF),
                pltpu.VMEM((layers, CHUNKS, tp, cr, q_dev), BF),
                pltpu.VMEM((layers, CHUNKS, tp, cr, q_dev), BF),
                pltpu.VMEM((layers, CHUNKS, tp, cr, q_dev), BF),
                pltpu.VMEM((hr, head_dim), BF),
                pltpu.VMEM((hr, slots), F32),
                pltpu.VMEM((hr, head_dim), F32),
                pltpu.VMEM((128, head_dim), F32),
                pltpu.VMEM((CHUNKS, cr, head_dim // 2), F32),
                pltpu.VMEM((CHUNKS, cr, head_dim // 2), F32),
                pltpu.VMEM((CHUNKS, cr, 1), F32),
                pltpu.VMEM((CHUNKS, hr, 1), F32),
                pltpu.VMEM((batch, batch), BF),
                pltpu.VMEM((shard, batch), BF),
                dma,
                dma((layers, 4)), dma((layers, 2)),
                dma((tp - 1,)), dma((tp - 1,)),
                dma((layers, CHUNKS, 7)), dma((layers, CHUNKS, tp)),
                dma((layers, CHUNKS, tp - 1)), dma((layers, CHUNKS, tp - 1)),
                dma((layers, CHUNKS, tp - 1)), dma((layers, CHUNKS, tp - 1)),
                dma((layers, CHUNKS, 4)), dma((layers, CHUNKS, 4)),
                dma((layers, CHUNKS, 3)), dma((layers, CHUNKS, 3)),
            ],
            compiler_params=pltpu.CompilerParams(collective_id=0, has_side_effects=True, vmem_limit_bytes=27 * 2 ** 20),
            name="step",
        )(residual.T, lengths[None, :], ln_scale, inv_freq, jnp.swapaxes(w_in, 1, 2), w_key, w_val, w_out, key_cache, val_cache)
        def swap(value, bit):
            return lax.ppermute(value, "tp", [(i, i ^ bit) for i in range(tp)])

        parts = [swap(sum_d, 6), swap(sum_x, 2), swap(sum_y, 4)]
        keep = functools.partial(pltpu.with_memory_space_constraint, memory_space=pltpu.VMEM)
        key_out, val_out = pl.pallas_call(
            cache_kernel,
            out_shape=[jax.ShapeDtypeStruct(key_cache.shape, BF)] * 2,
            in_specs=[smem] + [vmem] * 3,
            out_specs=[hbm, hbm],
            scratch_shapes=[pltpu.VMEM((layers, 2, rows, 16, head_dim), BF), dma((16,)), dma((16,))],
            compiler_params=pltpu.CompilerParams(vmem_limit_bytes=5 * 2 ** 20),
            name="caches",
        )(lengths, keep(new_k), keep(new_v), keep(kv_all))
        r_new = pl.pallas_call(
            functools.partial(final_kernel, cw, cr, rows),
            out_shape=jax.ShapeDtypeStruct((shard, batch), BF),
            in_specs=[vmem] * 4,
            out_specs=vmem,
            compiler_params=pltpu.CompilerParams(vmem_limit_bytes=8 * 2 ** 20),
            name="last",
        )(keep(base), *parts)
        return r_new.T, key_out, val_out

    cache_spec = P(None, ("dp", "tp"), None, None)
    return jax.shard_map(device_step, mesh=mesh, in_specs=(P("dp", "tp"), P(("dp", "tp")), P(None, "tp"), P(None, None, "tp"), P(), P(), P(None, "tp", None), cache_spec, cache_spec), out_specs=(P("dp", "tp"), cache_spec, cache_spec), check_vma=False)
```

```python
import functools

import jax
import jax.numpy as jnp
import numpy as np
from jax import lax
from jax.experimental import pallas as pl
from jax.experimental.pallas import tpu as pltpu
from jax.sharding import PartitionSpec as P

NORM_EPS = 1e-6
MESH = pl.DeviceIdType.MESH
CHUNKS = 2
BF = jnp.bfloat16
F32 = jnp.float32
TN = (((0,), (0,)), ((), ()))
NT = (((1,), (1,)), ((), ()))


def dot(a, b, dims=None):
    if dims is None:
        return jnp.dot(a, b, preferred_element_type=F32)
    return lax.dot_general(a, b, dims, preferred_element_type=F32)


def iota2(shape, dim):
    return lax.broadcasted_iota(jnp.int32, shape, dim)


def step_kernel(r_in, len_row, ln_in, inv_freq, w_in, w_key, w_val, w_out, k_cache, v_cache,
                sum_d, sum_x, sum_y, base, new_k, new_v, kv_all,
                w_in_v, w_key_v, w_val_v, w_out_v, w_out_t,
                r_all, ln_all, ln_col, h_t, joined, y_part, d2d, rs_recv, rs_send,
                q_send, q_recv, o_send, o_recv, q_rows, s_rows, o_rows, kv_tmp,
                cos_b, sin_b, len_col, len_rep, perm, r_buf, r_sem,
                w_sems, c_sems, ln_ss, ln_rs, ag_ss, ag_rs, q_ss, q_rs, o_ss, o_rs, d_ss, d_rs, t_ss, t_rs):
    layers, width = w_in.shape[0], w_in.shape[2]
    shard, batch = r_in.shape
    tp = width // shard
    rows = batch // tp
    q_dev = q_send.shape[2]
    ffn_dev = w_out.shape[1] - q_dev
    head_dim = w_key.shape[2]
    half = head_dim // 2
    heads = q_dev * tp // head_dim
    cw = batch // CHUNKS
    cr = rows // CHUNKS
    hr = cr * heads

    me = lax.axis_index("tp")
    core, xpos, ypos = me % 2, (me // 2) % 2, me // 4
    dp_ = me + 1 - 2 * core
    dx = me + 2 - 4 * xpos
    dy = me + 4 - 8 * ypos
    dd = dx + 4 - 8 * ypos
    flip = 1 - 2 * core

    def rcopy(src, dst, ss, rs, dev):
        return pltpu.make_async_remote_copy(src_ref=src, dst_ref=dst, send_sem=ss, recv_sem=rs,
                                            device_id={"tp": dev}, device_id_type=MESH)

    barrier = pltpu.get_barrier_semaphore()
    for off in range(1, tp):
        pl.semaphore_signal(barrier, 1, device_id={"tp": (me + off) % tp}, device_id_type=MESH)

    r_load = pltpu.make_async_copy(r_in, r_buf, r_sem)
    r_load.start()

    loads = {}

    def load(name, src, dst, sem):
        loads[name] = pltpu.make_async_copy(src, dst, sem)
        loads[name].start()

    def load_in(l):
        load(("key", l), w_key.at[l], w_key_v, w_sems.at[l, 1])
        load(("val", l), w_val.at[l], w_val_v, w_sems.at[l, 2])
        load(("in", l), w_in.at[l], w_in_v, w_sems.at[l, 0])

    def load_out(l):
        load(("out", l), w_out.at[l], w_out_v, w_sems.at[l, 3])

    def load_cache(l):
        load(("k", l), k_cache.at[l], kv_all.at[0, l], c_sems.at[l, 0])
        load(("v", l), v_cache.at[l], kv_all.at[1, l], c_sems.at[l, 1])

    perm[...] = order(cw, cr, rows, batch)
    r_load.wait()
    load_out(0)
    load_in(0)
    r_all[0, me] = dot(r_buf[...], perm[...]).astype(BF)
    ln_all[me] = ln_in[...]

    pl.semaphore_wait(barrier, tp - 1)

    def lanes(c):
        return pl.ds(c * cw, cw)

    def ag_send(l, c, kind, dev, slot):
        ref = r_all.at[l, slot, :, lanes(c)]
        rcopy(ref, ref, ag_ss.at[l], ag_rs.at[l, c, kind], dev).start()

    def got(ref, sem):
        rcopy(ref, ref, ln_ss, sem, dp_).wait_recv()

    def ag_start(l, c):
        ag_send(l, c, 2, dd, me)
        ag_send(l, c, 0, dx, me)
        ag_send(l, c, 1, dy, me)
        ag_send(l, c, 3, dp_, me)

    def ag_relay(l, c):
        for n, slot in enumerate((dx, dy, dd)):
            got(r_all.at[l, slot, :, lanes(c)], ag_rs.at[l, c, n])
            ag_send(l, c, 3, dp_, slot)

    def ag_finish(l, c):
        got(r_all.at[l, pl.ds(0, tp // 2), :, lanes(c)], ag_rs.at[l, c, 3])

    def ln_start():
        for off in range(1, tp):
            rcopy(ln_all.at[me], ln_all.at[me], ln_ss, ln_rs, (me + off) % tp).start()

    def ln_finish():
        got(ln_all.at[pl.ds(0, tp - 1)], ln_rs)
        for l in range(layers):
            pick = jnp.where(iota2((layers, 128), 0) == l, 1.0, 0.0).astype(BF)
            for s in range(tp):
                ln_col[l, s] = dot(ln_all[s], pick, TN)

    def setup_angles():
        lens = len_row[...].astype(F32)
        for c in range(CHUNKS):
            own = iota2((cr, rows), 1) == iota2((cr, rows), 0) + c * cr
            lc = jnp.sum(jnp.where(own, lens, 0.0), axis=1, keepdims=True)
            len_col[c] = lc
            rep = iota2((hr, rows), 1) == lax.shift_right_logical(iota2((hr, rows), 0), heads.bit_length() - 1) + c * cr
            len_rep[c] = jnp.sum(jnp.where(rep, lens, 0.0), axis=1, keepdims=True)
            ang = lc * inv_freq[...]
            cos_b[c] = jnp.cos(ang)
            sin_b[c] = jnp.sin(ang)

    def norm_query(l, c):
        cl = pl.ds(c * cw, cw)
        total = jnp.zeros((shard, cw), F32)
        squares = jnp.zeros((shard, cw), F32)
        for s in range(tp):
            v = r_all[l, s, :, cl].astype(F32)
            total = total + v
            squares = squares + v * v
        mean = jnp.sum(total, axis=0, keepdims=True) / width
        var = jnp.sum(squares, axis=0, keepdims=True) / width - mean * mean
        inv = lax.rsqrt(var + NORM_EPS)
        for s in range(tp):
            v = r_all[l, s, :, cl].astype(F32)
            scale = ln_col[l, s]
            scale = jnp.concatenate([scale] * (cw // 128), axis=1)
            h_t[pl.ds(s * shard, shard), cl] = ((v - mean) * inv * scale).astype(BF)
        q_t = dot(w_in_v[pl.ds(2 * ffn_dev, q_dev), :], h_t[:, cl])
        q_send[l, cl] = jnp.transpose(q_t).astype(BF)
        for off in range(1, tp):
            dev = (me + off) % tp
            rcopy(q_send.at[l, pl.ds(c * cw + dev * cr, cr)], q_recv.at[l, c, me], q_ss, q_rs.at[l, c], dev).start()
        q_recv[l, c, me] = q_send[l, pl.ds(pl.multiple_of(c * cw + me * cr, cr), cr)]

    def key_value(l, c):
        per = 128 // cr
        blk = h_t[:, pl.ds(pl.multiple_of(c * cw + (me // per) * 128, 128), 128)]
        here = pl.ds(pl.multiple_of((me % per) * cr, cr), cr)
        kv_tmp[...] = dot(blk, w_key_v[...], TN)
        k = kv_tmp[here].astype(BF).astype(F32)
        x1, x2 = k[:, :half], k[:, half:]
        co, si = cos_b[c], sin_b[c]
        new_k[l, pl.ds(c * cr, cr), :half] = (x1 * co - x2 * si).astype(BF).astype(F32)
        new_k[l, pl.ds(c * cr, cr), half:] = (x2 * co + x1 * si).astype(BF).astype(F32)
        kv_tmp[...] = dot(blk, w_val_v[...], TN)
        new_v[l, pl.ds(c * cr, cr)] = kv_tmp[here].astype(BF).astype(F32)

    def feed_forward(l, c):
        cl = pl.ds(c * cw, cw)
        tile = 432

        def body(i, _):
            o = pl.multiple_of(i * tile, 16)
            gate = dot(w_in_v[pl.ds(o, tile)], h_t[:, cl]).astype(BF).astype(F32)
            up = dot(w_in_v[pl.ds(o + ffn_dev, tile)], h_t[:, cl]).astype(BF).astype(F32)
            joined[pl.ds(o, tile), cl] = (gate * jax.nn.sigmoid(gate) * up).astype(BF)
            return 0

        lax.fori_loop(0, ffn_dev // tile, body, 0)

    def attention(l, c):
        got(q_recv.at[l, c, pl.ds(0, tp - 1)], q_rs.at[l, c])
        co, si = cos_b[c], sin_b[c]
        r1, r2 = [], []
        for h in range(heads):
            x1 = q_recv[l, c, 2 * h].astype(F32)
            x2 = q_recv[l, c, 2 * h + 1].astype(F32)
            r1.append((x1 * co - x2 * si).astype(BF))
            r2.append((x2 * co + x1 * si).astype(BF))
        ri, ci = iota2((hr, hr), 0), iota2((hr, hr), 1)
        mix = jnp.where(ci == (ri & (heads - 1)) * cr + lax.shift_right_logical(ri, heads.bit_length() - 1), 1.0, 0.0).astype(BF)
        q_rows[:, :half] = dot(mix, jnp.concatenate(r1, axis=0)).astype(BF)
        q_rows[:, half:] = dot(mix, jnp.concatenate(r2, axis=0)).astype(BF)
        rep = jnp.where(iota2((hr, cr), 1) == lax.shift_right_logical(iota2((hr, cr), 0), heads.bit_length() - 1), 1.0, 0.0).astype(BF)
        k_rep = dot(rep, new_k[l, pl.ds(c * cr, cr)].astype(BF))
        v_rep = dot(rep, new_v[l, pl.ds(c * cr, cr)].astype(BF))
        q_all = q_rows[...].astype(F32)
        s_new = jnp.sum(q_all * k_rep, axis=1, keepdims=True) * head_dim ** -0.5
        group = 16 // heads
        which = lax.shift_right_logical(iota2((16, head_dim), 0), heads.bit_length() - 1)
        if c == 0:
            loads[("k", l)].wait()

        def score(g, _):
            o = pl.multiple_of(g * 16, 16)
            qg = q_rows[pl.ds(o, 16)]
            acc = jnp.zeros((16, head_dim), F32)
            for j in range(group):
                acc = jnp.where(which == j, dot(qg, kv_all[0, l, c * cr + g * group + j], NT), acc)
            s_rows[pl.ds(o, 16)] = acc
            return 0

        lax.fori_loop(0, hr // 16, score, 0, unroll=4)
        s = s_rows[...] * head_dim ** -0.5
        pos = iota2((hr, s.shape[1]), 1).astype(F32)
        s = jnp.where(pos < len_rep[c], s, -1e30)
        top = jnp.maximum(jnp.max(s, axis=1, keepdims=True), s_new)
        w = jnp.exp(s - top)
        w_new = jnp.exp(s_new - top)
        total = jnp.sum(w, axis=1, keepdims=True) + w_new
        q_rows[...] = w.astype(BF)
        if c == 0:
            loads[("v", l)].wait()

        def mixv(g, _):
            o = pl.multiple_of(g * 16, 16)
            wg = q_rows[pl.ds(o, 16)]
            acc = jnp.zeros((16, head_dim), F32)
            for j in range(group):
                acc = jnp.where(which == j, dot(wg, kv_all[1, l, c * cr + g * group + j]), acc)
            o_rows[pl.ds(o, 16)] = acc
            return 0

        lax.fori_loop(0, hr // 16, mixv, 0, unroll=4)
        mixed = (o_rows[...] + w_new.astype(BF).astype(F32) * v_rep) / total
        back = jnp.where(ri == (ci & (heads - 1)) * cr + lax.shift_right_logical(ci, heads.bit_length() - 1), 1.0, 0.0).astype(BF)
        heads_o = dot(back, mixed.astype(BF)).astype(BF)
        for t in range(tp):
            o_send[l, c, t] = heads_o[(t // 2) * cr:(t // 2 + 1) * cr, (t % 2) * half:(t % 2 + 1) * half]
        for off in range(1, tp):
            dev = (me + off) % tp
            rcopy(o_send.at[l, c, dev], o_recv.at[l, c, me], o_ss, o_rs.at[l, c], dev).start()
        o_recv[l, c, me] = o_send[l, c, me]

    def project(l, c):
        cl = pl.ds(c * cw, cw)
        got(o_recv.at[l, c, pl.ds(0, tp - 1)], o_rs.at[l, c])
        o_all = jnp.concatenate([o_recv[l, c, j].astype(F32) for j in range(tp)], axis=0)
        joined[pl.ds(ffn_dev, q_dev), cl] = jnp.transpose(o_all).astype(BF)

        for n, slot in enumerate((dd + flip, dx + flip, dy + flip, me + flip, dd, dx, dy, me)):
            at = pl.ds(pl.multiple_of(slot * shard, 16), shard)
            y_part[l, at, cl] = dot(w_out_t[at], joined[:, cl]).astype(BF)
            if n < 4:
                rcopy(y_part.at[l, at, cl], d2d.at[l, slot // 2, :, cl], d_ss.at[l], d_rs.at[l, c], dp_).start()

    def turn_out(l):
        loads[("out", l)].wait()

        def body(i, _):
            o = pl.multiple_of(i * 128, 128)
            w_out_t[pl.ds(o, 128)] = jnp.transpose(w_out_v[:, pl.ds(o, 128)])
            return 0

        lax.fori_loop(0, width // 128, body, 0)

    def chip_sum(l, c, slot, n):
        if n == 0:
            got(d2d.at[l, :, :, lanes(c)], d_rs.at[l, c])
        mine = y_part[l, pl.ds(pl.multiple_of(slot * shard, 16), shard), lanes(c)].astype(F32)
        return mine + d2d[l, slot // 2, :, lanes(c)].astype(F32)

    def rs_first(l, c):
        for n, dev in enumerate((dd, dx, dy)):
            rs_send[l, c, n] = chip_sum(l, c, dev, n).astype(BF)
            rcopy(rs_send.at[l, c, n], rs_recv.at[l, c, n], t_ss, t_rs.at[l, c], dev).start()

    def chip_sums(l, c):
        for n, (out, dev) in enumerate(((sum_d, dd), (sum_x, dx), (sum_y, dy))):
            out[:, lanes(c)] = chip_sum(l, c, dev, n).astype(BF)
        base[:, lanes(c)] = r_all[l, me, :, lanes(c)].astype(F32) + chip_sum(l, c, me, 3)

    def rs_last(l, c):
        total = chip_sum(l, c, me, 3)
        got(rs_recv.at[l, c], t_rs.at[l, c])
        for n in range(3):
            total = total + rs_recv[l, c, n].astype(F32)
        return (r_all[l, me, :, lanes(c)].astype(F32) + total).astype(BF)

    def keep(l, c, part):
        r_all[l, me, :, lanes(c)] = part
        ag_start(l, c)

    ln_start()
    ag_start(0, 0)
    ag_start(0, 1)
    load_cache(0)
    setup_angles()
    turn_out(0)
    ag_relay(0, 0)
    ln_finish()
    ag_finish(0, 0)
    for l in range(layers):
        last = l + 1 == layers
        loads[("in", l)].wait()
        norm_query(l, 0)
        if not last:
            load_cache(l + 1)
        loads[("key", l)].wait()
        loads[("val", l)].wait()
        key_value(l, 0)
        if l == 0:
            ag_relay(l, 1)
            feed_forward(l, 0)
        else:
            feed_forward(l, 0)
            ag_relay(l, 1)
        ag_finish(l, 1)
        norm_query(l, 1)
        key_value(l, 1)
        attention(l, 0)
        feed_forward(l, 1)
        if not last:
            load_in(l + 1)
            load_out(l + 1)
        attention(l, 1)
        project(l, 0)
        if last:
            chip_sums(l, 0)
        else:
            rs_first(l, 0)
        project(l, 1)
        if last:
            chip_sums(l, 1)
        else:
            rs_first(l, 1)
            turn_out(l + 1)
            keep(l + 1, 0, rs_last(l, 0))
            keep(l + 1, 1, rs_last(l, 1))
            ag_relay(l + 1, 0)
            ag_finish(l + 1, 0)
    def sent(ref, sem):
        rcopy(ref, ref, sem, ln_rs, dp_).wait_send()

    sent(ln_all.at[pl.ds(0, tp - 1)], ln_ss)
    sent(q_send.at[:, pl.ds(0, CHUNKS * (tp - 1) * cr)], q_ss)
    sent(o_send.at[:, :, pl.ds(0, tp - 1)], o_ss)
    for l in range(layers):
        sent(r_all.at[l, pl.ds(0, tp - 1)], ag_ss.at[l])
        sent(y_part.at[l, pl.ds(0, width // 2)], d_ss.at[l])
    sent(rs_send, t_ss)


def order(cw, cr, rows, batch):
    pos = iota2((1, batch), 1)
    want = ((pos & (cw - 1)) // cr) * rows + (pos // cw) * cr + (pos & (cr - 1))
    return jnp.where(iota2((batch, batch), 0) == want, 1.0, 0.0).astype(BF)


def final_kernel(cw, cr, rows, base, part_d, part_x, part_y, out):
    total = base[...] + part_d[...].astype(F32) + part_x[...].astype(F32) + part_y[...].astype(F32)
    out[...] = dot(total.astype(BF), order(cw, cr, rows, base.shape[1]), NT).astype(BF)


def cache_kernel(lengths, new_k, new_v, kv_all, k_out, v_out, tiles, ends, big_sems, tile_sems):
    layers, rows = kv_all.shape[1:3]
    per = 16
    pairs = [(kv_all.at[0], k_out, new_k, 0), (kv_all.at[1], v_out, new_v, 1)]
    jobs = [(l, g, pair) for l in range(layers) for pair in pairs for g in range(rows // per)]

    n_tail = ends.shape[0]
    body = len(jobs) - n_tail

    def big(i):
        l, g, (src, dst, _, _) = jobs[i]
        at = pl.ds(g * per, per)
        return pltpu.make_async_copy(src.at[l, at] if i < body else ends.at[i - body], dst.at[l, at], big_sems.at[i])

    for i in range(body):
        big(i).start()
    for i in range(body, len(jobs)):
        l, g, (src, _, new, _) = jobs[i]

        def fill(j, _):
            b = g * per + j
            slot = lengths[b]
            base = pl.multiple_of((slot // 16) * 16, 16)
            hit = iota2((16, kv_all.shape[4]), 0) == slot - base
            ends[i - body, j] = src[l, b]
            old = src[l, b, pl.ds(base, 16)].astype(F32)
            ends[i - body, j, pl.ds(base, 16)] = jnp.where(hit, new[l, pl.ds(b, 1)], old).astype(BF)
            return 0

        lax.fori_loop(0, per, fill, 0)
        big(i).start()

    def build(b, _):
        slot = lengths[b]
        base = pl.multiple_of((slot // 16) * 16, 16)
        hit = iota2((16, kv_all.shape[4]), 0) == slot - base
        for l in range(layers):
            for src, _, new, n in pairs:
                old = src[l, b, pl.ds(base, 16)].astype(F32)
                tiles[l, n, b] = jnp.where(hit, new[l, pl.ds(b, 1)], old).astype(BF)
        return 0

    lax.fori_loop(0, rows, build, 0, unroll=4)
    for i in range(body):
        l, g, (_, dst, _, n) = jobs[i]
        big(i).wait()

        def patch(j, _):
            b = g * per + j
            base = pl.multiple_of((lengths[b] // 16) * 16, 16)
            pltpu.make_async_copy(tiles.at[l, n, b], dst.at[l, b, pl.ds(base, 16)], tile_sems.at[i]).start()
            return 0

        lax.fori_loop(0, per, patch, 0, unroll=4)
    for i in range(len(jobs)):
        if i >= body:
            big(i).wait()
            continue
        l, g, (_, dst, _, n) = jobs[i]
        at = pl.ds(g * per, per)
        pltpu.make_async_copy(tiles.at[l, n, at], dst.at[l, at, pl.ds(0, 16)], tile_sems.at[i]).wait()


def solution(mesh):
    tp = mesh.shape["tp"]

    def device_step(residual, lengths, ln_scale, w_in, w_key, w_val, w_out, key_cache, val_cache):
        layers, width, in_cols = w_in.shape
        batch, shard = residual.shape
        rows = lengths.shape[0]
        head_dim = w_key.shape[2]
        ffn_dev = in_cols - w_out.shape[1]
        q_dev = w_out.shape[1] - ffn_dev
        heads = q_dev * tp // head_dim
        cw, cr = batch // CHUNKS, rows // CHUNKS
        hr = cr * heads
        slots = key_cache.shape[2]
        inv_freq = jnp.asarray((10000.0 ** (-np.arange(head_dim // 2) * (2.0 / head_dim))).astype(np.float32))[None, :]
        vmem = pl.BlockSpec(memory_space=pltpu.VMEM)
        hbm = pl.BlockSpec(memory_space=pltpu.HBM)
        smem = pl.BlockSpec(memory_space=pltpu.SMEM)
        dma = pltpu.SemaphoreType.DMA
        sum_d, sum_x, sum_y, base, new_k, new_v, kv_all = pl.pallas_call(
            step_kernel,
            out_shape=[pltpu.VMEM((shard, batch), BF)] * 3 + [
                       pltpu.VMEM((shard, batch), F32),
                       pltpu.VMEM((layers, rows, head_dim), F32),
                       pltpu.VMEM((layers, rows, head_dim), F32),
                       pltpu.VMEM((2,) + key_cache.shape, BF)],
            in_specs=[hbm] + [vmem] * 3 + [hbm] * 6,
            out_specs=[vmem] * 7,
            scratch_shapes=[
                pltpu.VMEM((in_cols, width), BF),
                pltpu.VMEM((width, head_dim), BF),
                pltpu.VMEM((width, head_dim), BF),
                pltpu.VMEM((w_out.shape[1], width), BF),
                pltpu.VMEM((width, w_out.shape[1]), BF),
                pltpu.VMEM((layers, tp, shard, batch), BF),
                pltpu.VMEM((tp, layers, shard), BF),
                pltpu.VMEM((layers, tp, shard, 128), F32),
                pltpu.VMEM((width, batch), BF),
                pltpu.VMEM((ffn_dev + q_dev, batch), BF),
                pltpu.VMEM((layers, width, batch), BF),
                pltpu.VMEM((layers, tp // 2, shard, batch), BF),
                pltpu.VMEM((layers - 1, CHUNKS, 3, shard, cw), BF),
                pltpu.VMEM((layers - 1, CHUNKS, 3, shard, cw), BF),
                pltpu.VMEM((layers, batch, q_dev), BF),
                pltpu.VMEM((layers, CHUNKS, tp, cr, q_dev), BF),
                pltpu.VMEM((layers, CHUNKS, tp, cr, q_dev), BF),
                pltpu.VMEM((layers, CHUNKS, tp, cr, q_dev), BF),
                pltpu.VMEM((hr, head_dim), BF),
                pltpu.VMEM((hr, slots), F32),
                pltpu.VMEM((hr, head_dim), F32),
                pltpu.VMEM((128, head_dim), F32),
                pltpu.VMEM((CHUNKS, cr, head_dim // 2), F32),
                pltpu.VMEM((CHUNKS, cr, head_dim // 2), F32),
                pltpu.VMEM((CHUNKS, cr, 1), F32),
                pltpu.VMEM((CHUNKS, hr, 1), F32),
                pltpu.VMEM((batch, batch), BF),
                pltpu.VMEM((shard, batch), BF),
                dma,
                dma((layers, 4)), dma((layers, 2)),
                dma, dma,
                dma((layers,)), dma((layers, CHUNKS, 4)),
                dma, dma((layers, CHUNKS)),
                dma, dma((layers, CHUNKS)),
                dma((layers,)), dma((layers, CHUNKS)),
                dma, dma((layers - 1, CHUNKS)),
            ],
            compiler_params=pltpu.CompilerParams(collective_id=0, has_side_effects=True, vmem_limit_bytes=27 * 2 ** 20),
            name="step",
        )(residual.T, lengths[None, :], ln_scale, inv_freq, jnp.swapaxes(w_in, 1, 2), w_key, w_val, w_out, key_cache, val_cache)
        def swap(value, bit):
            return lax.ppermute(value, "tp", [(i, i ^ bit) for i in range(tp)])

        parts = [swap(sum_d, 6), swap(sum_x, 2), swap(sum_y, 4)]
        keep = functools.partial(pltpu.with_memory_space_constraint, memory_space=pltpu.VMEM)
        key_out, val_out = pl.pallas_call(
            cache_kernel,
            out_shape=[jax.ShapeDtypeStruct(key_cache.shape, BF)] * 2,
            in_specs=[smem] + [vmem] * 3,
            out_specs=[hbm, hbm],
            scratch_shapes=[pltpu.VMEM((layers, 2, rows, 16, head_dim), BF), pltpu.VMEM((2, 16, slots, head_dim), BF), dma((16,)), dma((14,))],
            compiler_params=pltpu.CompilerParams(vmem_limit_bytes=9 * 2 ** 20),
            name="caches",
        )(lengths, keep(new_k), keep(new_v), keep(kv_all))
        r_new = pl.pallas_call(
            functools.partial(final_kernel, cw, cr, rows),
            out_shape=jax.ShapeDtypeStruct((shard, batch), BF),
            in_specs=[vmem] * 4,
            out_specs=vmem,
            compiler_params=pltpu.CompilerParams(vmem_limit_bytes=8 * 2 ** 20),
            name="last",
        )(keep(base), *parts)
        return r_new.T, key_out, val_out

    cache_spec = P(None, ("dp", "tp"), None, None)
    return jax.shard_map(device_step, mesh=mesh, in_specs=(P("dp", "tp"), P(("dp", "tp")), P(None, "tp"), P(None, None, "tp"), P(), P(), P(None, "tp", None), cache_spec, cache_spec), out_specs=(P("dp", "tp"), cache_spec, cache_spec), check_vma=False)
```

```python
import functools

import jax
import jax.numpy as jnp
import numpy as np
from jax import lax
from jax.experimental import pallas as pl
from jax.experimental.pallas import tpu as pltpu
from jax.sharding import PartitionSpec as P

NORM_EPS = 1e-6
MESH = pl.DeviceIdType.MESH
CHUNKS = 2
BF = jnp.bfloat16
F32 = jnp.float32
TN = (((0,), (0,)), ((), ()))
NT = (((1,), (1,)), ((), ()))


def dot(a, b, dims=None):
    if dims is None:
        return jnp.dot(a, b, preferred_element_type=F32)
    return lax.dot_general(a, b, dims, preferred_element_type=F32)


def iota2(shape, dim):
    return lax.broadcasted_iota(jnp.int32, shape, dim)


def step_kernel(r_in, len_row, ln_in, inv_freq, w_in, w_key, w_val, w_out, k_cache, v_cache,
                sum_d, sum_x, sum_y, base, new_k, new_v, kv_all,
                w_in_v, w_key_v, w_val_v, w_out_v, w_out_t,
                r_all, ln_all, ln_col, h_t, joined, y_part, d2d, rs_recv, rs_send,
                q_send, q_recv, o_send, o_recv, q_rows, s_rows, o_rows, kv_tmp,
                cos_b, sin_b, len_col, len_rep, perm, r_buf, r_sem,
                w_sems, c_sems, ln_ss, ln_rs, ag_ss, ag_rs, q_ss, q_rs, o_ss, o_rs, d_ss, d_rs, t_ss, t_rs):
    layers, width = w_in.shape[0], w_in.shape[2]
    shard, batch = r_in.shape
    tp = width // shard
    rows = batch // tp
    q_dev = q_send.shape[2]
    ffn_dev = w_out.shape[1] - q_dev
    head_dim = w_key.shape[2]
    half = head_dim // 2
    heads = q_dev * tp // head_dim
    cw = batch // CHUNKS
    cr = rows // CHUNKS
    hr = cr * heads

    me = lax.axis_index("tp")
    core, xpos, ypos = me % 2, (me // 2) % 2, me // 4
    dp_ = me + 1 - 2 * core
    dx = me + 2 - 4 * xpos
    dy = me + 4 - 8 * ypos
    dd = dx + 4 - 8 * ypos
    flip = 1 - 2 * core

    def rcopy(src, dst, ss, rs, dev):
        return pltpu.make_async_remote_copy(src_ref=src, dst_ref=dst, send_sem=ss, recv_sem=rs,
                                            device_id={"tp": dev}, device_id_type=MESH)

    barrier = pltpu.get_barrier_semaphore()
    for off in range(1, tp):
        pl.semaphore_signal(barrier, 1, device_id={"tp": (me + off) % tp}, device_id_type=MESH)

    r_load = pltpu.make_async_copy(r_in, r_buf, r_sem)
    r_load.start()

    loads = {}

    def load(name, src, dst, sem):
        loads[name] = pltpu.make_async_copy(src, dst, sem)
        loads[name].start()

    def load_in(l):
        load(("key", l), w_key.at[l], w_key_v, w_sems.at[l, 1])
        load(("val", l), w_val.at[l], w_val_v, w_sems.at[l, 2])
        load(("in", l), w_in.at[l], w_in_v, w_sems.at[l, 0])

    def load_out(l):
        load(("out", l), w_out.at[l], w_out_v, w_sems.at[l, 3])

    def load_cache(l):
        load(("k", l), k_cache.at[l], kv_all.at[0, l], c_sems.at[l, 0])
        load(("v", l), v_cache.at[l], kv_all.at[1, l], c_sems.at[l, 1])

    perm[...] = order(cw, cr, rows, batch)
    r_load.wait()
    load_out(0)
    load_in(0)
    r_all[0, me] = dot(r_buf[...], perm[...]).astype(BF)
    ln_all[me] = ln_in[...]

    pl.semaphore_wait(barrier, tp - 1)

    def lanes(c):
        return pl.ds(c * cw, cw)

    def ag_send(l, c, kind, dev, slot):
        ref = r_all.at[l, slot, :, lanes(c)]
        rcopy(ref, ref, ag_ss.at[l], ag_rs.at[l, c, kind], dev).start()

    def got(ref, sem):
        rcopy(ref, ref, ln_ss, sem, dp_).wait_recv()

    def ag_start(l, c):
        ag_send(l, c, 2, dd, me)
        ag_send(l, c, 0, dx, me)
        ag_send(l, c, 1, dy, me)
        ag_send(l, c, 3, dp_, me)

    def ag_relay(l, c):
        for n, slot in enumerate((dx, dy, dd)):
            got(r_all.at[l, slot, :, lanes(c)], ag_rs.at[l, c, n])
            ag_send(l, c, 3, dp_, slot)

    def ag_finish(l, c):
        got(r_all.at[l, pl.ds(0, tp // 2), :, lanes(c)], ag_rs.at[l, c, 3])

    def ln_start():
        for off in range(1, tp):
            rcopy(ln_all.at[me], ln_all.at[me], ln_ss, ln_rs, (me + off) % tp).start()

    def ln_finish():
        got(ln_all.at[pl.ds(0, tp - 1)], ln_rs)
        for l in range(layers):
            pick = jnp.where(iota2((layers, 128), 0) == l, 1.0, 0.0).astype(BF)
            for s in range(tp):
                ln_col[l, s] = dot(ln_all[s], pick, TN)

    def setup_angles():
        lens = len_row[...].astype(F32)
        for c in range(CHUNKS):
            own = iota2((cr, rows), 1) == iota2((cr, rows), 0) + c * cr
            lc = jnp.sum(jnp.where(own, lens, 0.0), axis=1, keepdims=True)
            len_col[c] = lc
            rep = iota2((hr, rows), 1) == lax.shift_right_logical(iota2((hr, rows), 0), heads.bit_length() - 1) + c * cr
            len_rep[c] = jnp.sum(jnp.where(rep, lens, 0.0), axis=1, keepdims=True)
            ang = lc * inv_freq[...]
            cos_b[c] = jnp.cos(ang)
            sin_b[c] = jnp.sin(ang)

    def norm_query(l, c):
        cl = pl.ds(c * cw, cw)
        total = jnp.zeros((shard, cw), F32)
        squares = jnp.zeros((shard, cw), F32)
        for s in range(tp):
            v = r_all[l, s, :, cl].astype(F32)
            total = total + v
            squares = squares + v * v
        mean = jnp.sum(total, axis=0, keepdims=True) / width
        var = jnp.sum(squares, axis=0, keepdims=True) / width - mean * mean
        inv = lax.rsqrt(var + NORM_EPS)
        for s in range(tp):
            v = r_all[l, s, :, cl].astype(F32)
            scale = ln_col[l, s]
            scale = jnp.concatenate([scale] * (cw // 128), axis=1)
            h_t[pl.ds(s * shard, shard), cl] = ((v - mean) * inv * scale).astype(BF)
        q_t = dot(w_in_v[pl.ds(2 * ffn_dev, q_dev), :], h_t[:, cl])
        q_send[l, cl] = jnp.transpose(q_t).astype(BF)
        for off in range(1, tp):
            dev = (me + off) % tp
            rcopy(q_send.at[l, pl.ds(c * cw + dev * cr, cr)], q_recv.at[l, c, me], q_ss, q_rs.at[l, c], dev).start()
        q_recv[l, c, me] = q_send[l, pl.ds(pl.multiple_of(c * cw + me * cr, cr), cr)]

    def key_value(l, c):
        per = 128 // cr
        blk = h_t[:, pl.ds(pl.multiple_of(c * cw + (me // per) * 128, 128), 128)]
        here = pl.ds(pl.multiple_of((me % per) * cr, cr), cr)
        kv_tmp[...] = dot(blk, w_key_v[...], TN)
        k = kv_tmp[here].astype(BF).astype(F32)
        x1, x2 = k[:, :half], k[:, half:]
        co, si = cos_b[c], sin_b[c]
        new_k[l, pl.ds(c * cr, cr), :half] = (x1 * co - x2 * si).astype(BF).astype(F32)
        new_k[l, pl.ds(c * cr, cr), half:] = (x2 * co + x1 * si).astype(BF).astype(F32)
        kv_tmp[...] = dot(blk, w_val_v[...], TN)
        new_v[l, pl.ds(c * cr, cr)] = kv_tmp[here].astype(BF).astype(F32)

    def feed_forward(l, c):
        cl = pl.ds(c * cw, cw)
        gate = dot(w_in_v[pl.ds(0, ffn_dev)], h_t[:, cl]).astype(BF).astype(F32)
        up = dot(w_in_v[pl.ds(ffn_dev, ffn_dev)], h_t[:, cl]).astype(BF).astype(F32)
        joined[pl.ds(0, ffn_dev), cl] = (gate * jax.nn.sigmoid(gate) * up).astype(BF)

    def attention(l, c):
        got(q_recv.at[l, c, pl.ds(0, tp - 1)], q_rs.at[l, c])
        co, si = cos_b[c], sin_b[c]
        r1, r2 = [], []
        for h in range(heads):
            x1 = q_recv[l, c, 2 * h].astype(F32)
            x2 = q_recv[l, c, 2 * h + 1].astype(F32)
            r1.append((x1 * co - x2 * si).astype(BF))
            r2.append((x2 * co + x1 * si).astype(BF))
        ri, ci = iota2((hr, hr), 0), iota2((hr, hr), 1)
        mix = jnp.where(ci == (ri & (heads - 1)) * cr + lax.shift_right_logical(ri, heads.bit_length() - 1), 1.0, 0.0).astype(BF)
        q_rows[:, :half] = dot(mix, jnp.concatenate(r1, axis=0)).astype(BF)
        q_rows[:, half:] = dot(mix, jnp.concatenate(r2, axis=0)).astype(BF)
        rep = jnp.where(iota2((hr, cr), 1) == lax.shift_right_logical(iota2((hr, cr), 0), heads.bit_length() - 1), 1.0, 0.0).astype(BF)
        k_rep = dot(rep, new_k[l, pl.ds(c * cr, cr)].astype(BF))
        v_rep = dot(rep, new_v[l, pl.ds(c * cr, cr)].astype(BF))
        q_all = q_rows[...].astype(F32)
        s_new = jnp.sum(q_all * k_rep, axis=1, keepdims=True) * head_dim ** -0.5
        group = 16 // heads
        which = lax.shift_right_logical(iota2((16, head_dim), 0), heads.bit_length() - 1)
        if c == 0:
            loads[("k", l)].wait()

        def score(g, _):
            o = pl.multiple_of(g * 16, 16)
            qg = q_rows[pl.ds(o, 16)]
            acc = jnp.zeros((16, head_dim), F32)
            for j in range(group):
                acc = jnp.where(which == j, dot(qg, kv_all[0, l, c * cr + g * group + j], NT), acc)
            s_rows[pl.ds(o, 16)] = acc
            return 0

        lax.fori_loop(0, hr // 16, score, 0, unroll=hr // 16)
        s = s_rows[...] * head_dim ** -0.5
        pos = iota2((hr, s.shape[1]), 1).astype(F32)
        s = jnp.where(pos < len_rep[c], s, -1e30)
        top = jnp.maximum(jnp.max(s, axis=1, keepdims=True), s_new)
        w = jnp.exp(s - top)
        w_new = jnp.exp(s_new - top)
        total = jnp.sum(w, axis=1, keepdims=True) + w_new
        q_rows[...] = w.astype(BF)
        if c == 0:
            loads[("v", l)].wait()

        def mixv(g, _):
            o = pl.multiple_of(g * 16, 16)
            wg = q_rows[pl.ds(o, 16)]
            acc = jnp.zeros((16, head_dim), F32)
            for j in range(group):
                acc = jnp.where(which == j, dot(wg, kv_all[1, l, c * cr + g * group + j]), acc)
            o_rows[pl.ds(o, 16)] = acc
            return 0

        lax.fori_loop(0, hr // 16, mixv, 0, unroll=hr // 16)
        mixed = (o_rows[...] + w_new.astype(BF).astype(F32) * v_rep) / total
        back = jnp.where(ri == (ci & (heads - 1)) * cr + lax.shift_right_logical(ci, heads.bit_length() - 1), 1.0, 0.0).astype(BF)
        heads_o = dot(back, mixed.astype(BF)).astype(BF)
        for t in range(tp):
            o_send[l, c, t] = heads_o[(t // 2) * cr:(t // 2 + 1) * cr, (t % 2) * half:(t % 2 + 1) * half]
        for off in range(1, tp):
            dev = (me + off) % tp
            rcopy(o_send.at[l, c, dev], o_recv.at[l, c, me], o_ss, o_rs.at[l, c], dev).start()
        o_recv[l, c, me] = o_send[l, c, me]

    def project(l, c):
        cl = pl.ds(c * cw, cw)
        got(o_recv.at[l, c, pl.ds(0, tp - 1)], o_rs.at[l, c])
        o_all = jnp.concatenate([o_recv[l, c, j].astype(F32) for j in range(tp)], axis=0)
        joined[pl.ds(ffn_dev, q_dev), cl] = jnp.transpose(o_all).astype(BF)

        for n, slot in enumerate((dd + flip, dx + flip, dy + flip, me + flip, dd, dx, dy, me)):
            at = pl.ds(pl.multiple_of(slot * shard, 16), shard)
            y_part[l, at, cl] = dot(w_out_t[at], joined[:, cl]).astype(BF)
            if n < 4:
                rcopy(y_part.at[l, at, cl], d2d.at[l, slot // 2, :, cl], d_ss.at[l], d_rs.at[l, c], dp_).start()

    def turn_out(l):
        loads[("out", l)].wait()

        def body(i, _):
            o = pl.multiple_of(i * 128, 128)
            w_out_t[pl.ds(o, 128)] = jnp.transpose(w_out_v[:, pl.ds(o, 128)])
            return 0

        lax.fori_loop(0, width // 128, body, 0)

    def chip_sum(l, c, slot, n):
        if n == 0:
            got(d2d.at[l, :, :, lanes(c)], d_rs.at[l, c])
        mine = y_part[l, pl.ds(pl.multiple_of(slot * shard, 16), shard), lanes(c)].astype(F32)
        return mine + d2d[l, slot // 2, :, lanes(c)].astype(F32)

    def rs_first(l, c):
        for n, dev in enumerate((dd, dx, dy)):
            rs_send[l, c, n] = chip_sum(l, c, dev, n).astype(BF)
            rcopy(rs_send.at[l, c, n], rs_recv.at[l, c, n], t_ss, t_rs.at[l, c], dev).start()

    def chip_sums(l, c):
        for n, (out, dev) in enumerate(((sum_d, dd), (sum_x, dx), (sum_y, dy))):
            out[:, lanes(c)] = chip_sum(l, c, dev, n).astype(BF)
        base[:, lanes(c)] = r_all[l, me, :, lanes(c)].astype(F32) + chip_sum(l, c, me, 3)

    def rs_last(l, c):
        total = chip_sum(l, c, me, 3)
        got(rs_recv.at[l, c], t_rs.at[l, c])
        for n in range(3):
            total = total + rs_recv[l, c, n].astype(F32)
        return (r_all[l, me, :, lanes(c)].astype(F32) + total).astype(BF)

    def keep(l, c, part):
        r_all[l, me, :, lanes(c)] = part
        ag_start(l, c)

    ln_start()
    ag_start(0, 0)
    ag_start(0, 1)
    load_cache(0)
    setup_angles()
    turn_out(0)
    ag_relay(0, 0)
    ln_finish()
    ag_finish(0, 0)
    for l in range(layers):
        last = l + 1 == layers
        loads[("in", l)].wait()
        norm_query(l, 0)
        if not last:
            load_cache(l + 1)
        loads[("key", l)].wait()
        loads[("val", l)].wait()
        key_value(l, 0)
        if l == 0:
            ag_relay(l, 1)
            feed_forward(l, 0)
        else:
            feed_forward(l, 0)
            ag_relay(l, 1)
        ag_finish(l, 1)
        norm_query(l, 1)
        key_value(l, 1)
        attention(l, 0)
        if not last:
            feed_forward(l, 1)
            load_in(l + 1)
            load_out(l + 1)
        attention(l, 1)
        if last:
            feed_forward(l, 1)
        project(l, 0)
        if last:
            project(l, 1)
            chip_sums(l, 0)
            chip_sums(l, 1)
        else:
            rs_first(l, 0)
            project(l, 1)
            rs_first(l, 1)
            keep(l + 1, 0, rs_last(l, 0))
            turn_out(l + 1)
            keep(l + 1, 1, rs_last(l, 1))
            ag_relay(l + 1, 0)
            ag_finish(l + 1, 0)

    def sent(ref, sem):
        rcopy(ref, ref, sem, ln_rs, dp_).wait_send()

    sent(ln_all.at[pl.ds(0, tp - 1)], ln_ss)
    sent(q_send.at[:, pl.ds(0, CHUNKS * (tp - 1) * cr)], q_ss)
    sent(o_send.at[:, :, pl.ds(0, tp - 1)], o_ss)
    for l in range(layers):
        sent(r_all.at[l, pl.ds(0, tp - 1)], ag_ss.at[l])
        sent(y_part.at[l, pl.ds(0, width // 2)], d_ss.at[l])
    sent(rs_send, t_ss)


def order(cw, cr, rows, batch):
    pos = iota2((1, batch), 1)
    want = ((pos & (cw - 1)) // cr) * rows + (pos // cw) * cr + (pos & (cr - 1))
    return jnp.where(iota2((batch, batch), 0) == want, 1.0, 0.0).astype(BF)


def final_kernel(cw, cr, rows, base, part_d, part_x, part_y, out):
    total = base[...] + part_d[...].astype(F32) + part_x[...].astype(F32) + part_y[...].astype(F32)
    out[...] = dot(total.astype(BF), order(cw, cr, rows, base.shape[1]), NT).astype(BF)


def cache_kernel(lengths, new_k, new_v, kv_all, k_out, v_out, tiles, ends, big_sems, tile_sems):
    layers, rows = kv_all.shape[1:3]
    per = 16
    pairs = [(kv_all.at[0], k_out, new_k, 0), (kv_all.at[1], v_out, new_v, 1)]
    jobs = [(l, g, pair) for l in range(layers) for pair in pairs for g in range(rows // per)]

    n_tail = ends.shape[0]
    body = len(jobs) - n_tail

    def big(i):
        l, g, (src, dst, _, _) = jobs[i]
        at = pl.ds(g * per, per)
        return pltpu.make_async_copy(src.at[l, at] if i < body else ends.at[i - body], dst.at[l, at], big_sems.at[i])

    for i in range(body):
        big(i).start()
    for i in range(body, len(jobs)):
        l, g, (src, _, new, _) = jobs[i]

        def fill(j, _):
            b = g * per + j
            slot = lengths[b]
            base = pl.multiple_of((slot // 16) * 16, 16)
            hit = iota2((16, kv_all.shape[4]), 0) == slot - base
            ends[i - body, j] = src[l, b]
            old = src[l, b, pl.ds(base, 16)].astype(F32)
            ends[i - body, j, pl.ds(base, 16)] = jnp.where(hit, new[l, pl.ds(b, 1)], old).astype(BF)
            return 0

        lax.fori_loop(0, per, fill, 0)
        big(i).start()

    def build(b, _):
        slot = lengths[b]
        base = pl.multiple_of((slot // 16) * 16, 16)
        hit = iota2((16, kv_all.shape[4]), 0) == slot - base
        for l in range(layers):
            for src, _, new, n in pairs:
                old = src[l, b, pl.ds(base, 16)].astype(F32)
                tiles[l, n, b] = jnp.where(hit, new[l, pl.ds(b, 1)], old).astype(BF)
        return 0

    lax.fori_loop(0, rows, build, 0, unroll=4)
    for i in range(body):
        l, g, (_, dst, _, n) = jobs[i]
        big(i).wait()

        def patch(j, _):
            b = g * per + j
            base = pl.multiple_of((lengths[b] // 16) * 16, 16)
            pltpu.make_async_copy(tiles.at[l, n, b], dst.at[l, b, pl.ds(base, 16)], tile_sems.at[i]).start()
            return 0

        lax.fori_loop(0, per, patch, 0, unroll=4)
    for i in range(len(jobs)):
        if i >= body:
            big(i).wait()
            continue
        l, g, (_, dst, _, n) = jobs[i]
        at = pl.ds(g * per, per)
        pltpu.make_async_copy(tiles.at[l, n, at], dst.at[l, at, pl.ds(0, 16)], tile_sems.at[i]).wait()


def solution(mesh):
    tp = mesh.shape["tp"]

    def device_step(residual, lengths, ln_scale, w_in, w_key, w_val, w_out, key_cache, val_cache):
        layers, width, in_cols = w_in.shape
        batch, shard = residual.shape
        rows = lengths.shape[0]
        head_dim = w_key.shape[2]
        ffn_dev = in_cols - w_out.shape[1]
        q_dev = w_out.shape[1] - ffn_dev
        heads = q_dev * tp // head_dim
        cw, cr = batch // CHUNKS, rows // CHUNKS
        hr = cr * heads
        slots = key_cache.shape[2]
        inv_freq = jnp.asarray((10000.0 ** (-np.arange(head_dim // 2) * (2.0 / head_dim))).astype(np.float32))[None, :]
        vmem = pl.BlockSpec(memory_space=pltpu.VMEM)
        hbm = pl.BlockSpec(memory_space=pltpu.HBM)
        smem = pl.BlockSpec(memory_space=pltpu.SMEM)
        dma = pltpu.SemaphoreType.DMA
        sum_d, sum_x, sum_y, base, new_k, new_v, kv_all = pl.pallas_call(
            step_kernel,
            out_shape=[pltpu.VMEM((shard, batch), BF)] * 3 + [
                       pltpu.VMEM((shard, batch), F32),
                       pltpu.VMEM((layers, rows, head_dim), F32),
                       pltpu.VMEM((layers, rows, head_dim), F32),
                       pltpu.VMEM((2,) + key_cache.shape, BF)],
            in_specs=[hbm] + [vmem] * 3 + [hbm] * 6,
            out_specs=[vmem] * 7,
            scratch_shapes=[
                pltpu.VMEM((in_cols, width), BF),
                pltpu.VMEM((width, head_dim), BF),
                pltpu.VMEM((width, head_dim), BF),
                pltpu.VMEM((w_out.shape[1], width), BF),
                pltpu.VMEM((width, w_out.shape[1]), BF),
                pltpu.VMEM((layers, tp, shard, batch), BF),
                pltpu.VMEM((tp, layers, shard), BF),
                pltpu.VMEM((layers, tp, shard, 128), F32),
                pltpu.VMEM((width, batch), BF),
                pltpu.VMEM((ffn_dev + q_dev, batch), BF),
                pltpu.VMEM((layers, width, batch), BF),
                pltpu.VMEM((layers, tp // 2, shard, batch), BF),
                pltpu.VMEM((layers - 1, CHUNKS, 3, shard, cw), BF),
                pltpu.VMEM((layers - 1, CHUNKS, 3, shard, cw), BF),
                pltpu.VMEM((layers, batch, q_dev), BF),
                pltpu.VMEM((layers, CHUNKS, tp, cr, q_dev), BF),
                pltpu.VMEM((layers, CHUNKS, tp, cr, q_dev), BF),
                pltpu.VMEM((layers, CHUNKS, tp, cr, q_dev), BF),
                pltpu.VMEM((hr, head_dim), BF),
                pltpu.VMEM((hr, slots), F32),
                pltpu.VMEM((hr, head_dim), F32),
                pltpu.VMEM((128, head_dim), F32),
                pltpu.VMEM((CHUNKS, cr, head_dim // 2), F32),
                pltpu.VMEM((CHUNKS, cr, head_dim // 2), F32),
                pltpu.VMEM((CHUNKS, cr, 1), F32),
                pltpu.VMEM((CHUNKS, hr, 1), F32),
                pltpu.VMEM((batch, batch), BF),
                pltpu.VMEM((shard, batch), BF),
                dma,
                dma((layers, 4)), dma((layers, 2)),
                dma, dma,
                dma((layers,)), dma((layers, CHUNKS, 4)),
                dma, dma((layers, CHUNKS)),
                dma, dma((layers, CHUNKS)),
                dma((layers,)), dma((layers, CHUNKS)),
                dma, dma((layers - 1, CHUNKS)),
            ],
            compiler_params=pltpu.CompilerParams(collective_id=0, has_side_effects=True, vmem_limit_bytes=27 * 2 ** 20),
            name="step",
        )(residual.T, lengths[None, :], ln_scale, inv_freq, jnp.swapaxes(w_in, 1, 2), w_key, w_val, w_out, key_cache, val_cache)
        def swap(value, bit):
            return lax.ppermute(value, "tp", [(i, i ^ bit) for i in range(tp)])

        parts = [swap(sum_d, 6), swap(sum_x, 2), swap(sum_y, 4)]
        keep = functools.partial(pltpu.with_memory_space_constraint, memory_space=pltpu.VMEM)
        key_out, val_out = pl.pallas_call(
            cache_kernel,
            out_shape=[jax.ShapeDtypeStruct(key_cache.shape, BF)] * 2,
            in_specs=[smem] + [vmem] * 3,
            out_specs=[hbm, hbm],
            scratch_shapes=[pltpu.VMEM((layers, 2, rows, 16, head_dim), BF), pltpu.VMEM((2, 16, slots, head_dim), BF), dma((16,)), dma((14,))],
            compiler_params=pltpu.CompilerParams(vmem_limit_bytes=9 * 2 ** 20),
            name="caches",
        )(lengths, keep(new_k), keep(new_v), keep(kv_all))
        r_new = pl.pallas_call(
            functools.partial(final_kernel, cw, cr, rows),
            out_shape=jax.ShapeDtypeStruct((shard, batch), BF),
            in_specs=[vmem] * 4,
            out_specs=vmem,
            compiler_params=pltpu.CompilerParams(vmem_limit_bytes=8 * 2 ** 20),
            name="last",
        )(keep(base), *parts)
        return r_new.T, key_out, val_out

    cache_spec = P(None, ("dp", "tp"), None, None)
    return jax.shard_map(device_step, mesh=mesh, in_specs=(P("dp", "tp"), P(("dp", "tp")), P(None, "tp"), P(None, None, "tp"), P(), P(), P(None, "tp", None), cache_spec, cache_spec), out_specs=(P("dp", "tp"), cache_spec, cache_spec), check_vma=False)
```

```python
import functools

import jax
import jax.numpy as jnp
import numpy as np
from jax import lax
from jax.experimental import pallas as pl
from jax.experimental.pallas import tpu as pltpu
from jax.sharding import PartitionSpec as P

NORM_EPS = 1e-6
MESH = pl.DeviceIdType.MESH
CHUNKS = 2
BF = jnp.bfloat16
F32 = jnp.float32
TN = (((0,), (0,)), ((), ()))
NT = (((1,), (1,)), ((), ()))


def dot(a, b, dims=None):
    if dims is None:
        return jnp.dot(a, b, preferred_element_type=F32)
    return lax.dot_general(a, b, dims, preferred_element_type=F32)


def iota2(shape, dim):
    return lax.broadcasted_iota(jnp.int32, shape, dim)


def step_kernel(r_in, len_row, ln_in, inv_freq, w_in, w_key, w_val, w_out, k_cache, v_cache,
                sum_d, sum_x, sum_y, base, new_k, new_v, kv_all,
                w_in_v, w_key_v, w_val_v, w_out_v, w_out_t,
                r_all, ln_all, ln_col, h_t, joined, y_part, d2d, rs_recv, rs_send,
                q_send, q_recv, o_send, o_recv, q_rows, s_rows, o_rows, kv_tmp,
                cos_b, sin_b, len_col, len_rep, perm, r_buf, r_sem,
                w_sems, c_sems, ln_ss, ln_rs, ag_ss, ag_rs, q_ss, q_rs, o_ss, o_rs, d_ss, d_rs, t_ss, t_rs):
    layers, width = w_in.shape[0], w_in.shape[2]
    shard, batch = r_in.shape
    tp = width // shard
    rows = batch // tp
    q_dev = q_send.shape[2]
    ffn_dev = w_out.shape[1] - q_dev
    head_dim = w_key.shape[2]
    half = head_dim // 2
    heads = q_dev * tp // head_dim
    cw = batch // CHUNKS
    cr = rows // CHUNKS
    hr = cr * heads

    me = lax.axis_index("tp")
    core, xpos, ypos = me % 2, (me // 2) % 2, me // 4
    dp_ = me + 1 - 2 * core
    dx = me + 2 - 4 * xpos
    dy = me + 4 - 8 * ypos
    dd = dx + 4 - 8 * ypos
    flip = 1 - 2 * core
    others = (dd + flip, dd, dx + flip, dy + flip, dx, dy, dp_)

    def rcopy(src, dst, ss, rs, dev):
        return pltpu.make_async_remote_copy(src_ref=src, dst_ref=dst, send_sem=ss, recv_sem=rs,
                                            device_id={"tp": dev}, device_id_type=MESH)

    barrier = pltpu.get_barrier_semaphore()
    for off in range(1, tp):
        pl.semaphore_signal(barrier, 1, device_id={"tp": (me + off) % tp}, device_id_type=MESH)

    r_load = pltpu.make_async_copy(r_in, r_buf, r_sem)
    r_load.start()

    loads = {}

    def load(name, src, dst, sem):
        loads[name] = pltpu.make_async_copy(src, dst, sem)
        loads[name].start()

    def load_in(l):
        load(("key", l), w_key.at[l], w_key_v, w_sems.at[l, 1])
        load(("val", l), w_val.at[l], w_val_v, w_sems.at[l, 2])
        load(("in", l), w_in.at[l], w_in_v, w_sems.at[l, 0])

    def load_out(l):
        load(("out", l), w_out.at[l], w_out_v, w_sems.at[l, 3])

    def load_cache(l):
        load(("k", l), k_cache.at[l], kv_all.at[0, l], c_sems.at[l, 0])
        load(("v", l), v_cache.at[l], kv_all.at[1, l], c_sems.at[l, 1])

    perm[...] = order(cw, cr, rows, batch)
    r_load.wait()
    load_out(0)
    load_in(0)
    r_all[0, me] = dot(r_buf[...], perm[...]).astype(BF)
    ln_all[me] = ln_in[...]

    pl.semaphore_wait(barrier, tp - 1)

    def lanes(c):
        return pl.ds(c * cw, cw)

    def ag_send(l, c, kind, dev, slot):
        ref = r_all.at[l, slot, :, lanes(c)]
        rcopy(ref, ref, ag_ss.at[l], ag_rs.at[l, c, kind], dev).start()

    def got(ref, sem):
        rcopy(ref, ref, ln_ss, sem, dp_).wait_recv()

    def ag_start(l, c):
        ag_send(l, c, 2, dd, me)
        ag_send(l, c, 0, dx, me)
        ag_send(l, c, 1, dy, me)
        ag_send(l, c, 3, dp_, me)

    def ag_relay(l, c):
        for n, slot in enumerate((dx, dy, dd)):
            got(r_all.at[l, slot, :, lanes(c)], ag_rs.at[l, c, n])
            ag_send(l, c, 3, dp_, slot)

    def ag_finish(l, c):
        got(r_all.at[l, pl.ds(0, tp // 2), :, lanes(c)], ag_rs.at[l, c, 3])

    def ln_start():
        for off in range(1, tp):
            rcopy(ln_all.at[me], ln_all.at[me], ln_ss, ln_rs, (me + off) % tp).start()

    def ln_finish():
        got(ln_all.at[pl.ds(0, tp - 1)], ln_rs)
        for l in range(layers):
            pick = jnp.where(iota2((layers, 128), 0) == l, 1.0, 0.0).astype(BF)
            for s in range(tp):
                ln_col[l, s] = dot(ln_all[s], pick, TN)

    def setup_angles():
        lens = len_row[...].astype(F32)
        for c in range(CHUNKS):
            own = iota2((cr, rows), 1) == iota2((cr, rows), 0) + c * cr
            lc = jnp.sum(jnp.where(own, lens, 0.0), axis=1, keepdims=True)
            len_col[c] = lc
            rep = iota2((hr, rows), 1) == lax.shift_right_logical(iota2((hr, rows), 0), heads.bit_length() - 1) + c * cr
            len_rep[c] = jnp.sum(jnp.where(rep, lens, 0.0), axis=1, keepdims=True)
            ang = lc * inv_freq[...]
            cos_b[c] = jnp.cos(ang)
            sin_b[c] = jnp.sin(ang)

    def norm_query(l, c):
        cl = pl.ds(c * cw, cw)
        total = jnp.zeros((shard, cw), F32)
        squares = jnp.zeros((shard, cw), F32)
        for s in range(tp):
            v = r_all[l, s, :, cl].astype(F32)
            total = total + v
            squares = squares + v * v
        mean = jnp.sum(total, axis=0, keepdims=True) / width
        var = jnp.sum(squares, axis=0, keepdims=True) / width - mean * mean
        inv = lax.rsqrt(var + NORM_EPS)
        for s in range(tp):
            v = r_all[l, s, :, cl].astype(F32)
            scale = ln_col[l, s]
            scale = jnp.concatenate([scale] * (cw // 128), axis=1)
            h_t[pl.ds(s * shard, shard), cl] = ((v - mean) * inv * scale).astype(BF)
        q_t = dot(w_in_v[pl.ds(2 * ffn_dev, q_dev), :], h_t[:, cl])
        q_send[l, cl] = jnp.transpose(q_t).astype(BF)
        for dev in others:
            rcopy(q_send.at[l, pl.ds(c * cw + dev * cr, cr)], q_recv.at[l, c, me], q_ss, q_rs.at[l, c], dev).start()
        q_recv[l, c, me] = q_send[l, pl.ds(pl.multiple_of(c * cw + me * cr, cr), cr)]

    def key_value(l, c):
        per = 128 // cr
        blk = h_t[:, pl.ds(pl.multiple_of(c * cw + (me // per) * 128, 128), 128)]
        here = pl.ds(pl.multiple_of((me % per) * cr, cr), cr)
        kv_tmp[...] = dot(blk, w_key_v[...], TN)
        k = kv_tmp[here].astype(BF).astype(F32)
        x1, x2 = k[:, :half], k[:, half:]
        co, si = cos_b[c], sin_b[c]
        new_k[l, pl.ds(c * cr, cr), :half] = (x1 * co - x2 * si).astype(BF).astype(F32)
        new_k[l, pl.ds(c * cr, cr), half:] = (x2 * co + x1 * si).astype(BF).astype(F32)
        kv_tmp[...] = dot(blk, w_val_v[...], TN)
        new_v[l, pl.ds(c * cr, cr)] = kv_tmp[here].astype(BF).astype(F32)

    def feed_forward(l, c):
        cl = pl.ds(c * cw, cw)
        gate = dot(w_in_v[pl.ds(0, ffn_dev)], h_t[:, cl]).astype(BF).astype(F32)
        up = dot(w_in_v[pl.ds(ffn_dev, ffn_dev)], h_t[:, cl]).astype(BF).astype(F32)
        joined[pl.ds(0, ffn_dev), cl] = (gate * jax.nn.sigmoid(gate) * up).astype(BF)

    def attention(l, c):
        got(q_recv.at[l, c, pl.ds(0, tp - 1)], q_rs.at[l, c])
        co, si = cos_b[c], sin_b[c]
        r1, r2 = [], []
        for h in range(heads):
            x1 = q_recv[l, c, 2 * h].astype(F32)
            x2 = q_recv[l, c, 2 * h + 1].astype(F32)
            r1.append((x1 * co - x2 * si).astype(BF))
            r2.append((x2 * co + x1 * si).astype(BF))
        ri, ci = iota2((hr, hr), 0), iota2((hr, hr), 1)
        mix = jnp.where(ci == (ri & (heads - 1)) * cr + lax.shift_right_logical(ri, heads.bit_length() - 1), 1.0, 0.0).astype(BF)
        q_rows[:, :half] = dot(mix, jnp.concatenate(r1, axis=0)).astype(BF)
        q_rows[:, half:] = dot(mix, jnp.concatenate(r2, axis=0)).astype(BF)
        rep = jnp.where(iota2((hr, cr), 1) == lax.shift_right_logical(iota2((hr, cr), 0), heads.bit_length() - 1), 1.0, 0.0).astype(BF)
        k_rep = dot(rep, new_k[l, pl.ds(c * cr, cr)].astype(BF))
        v_rep = dot(rep, new_v[l, pl.ds(c * cr, cr)].astype(BF))
        q_all = q_rows[...].astype(F32)
        s_new = jnp.sum(q_all * k_rep, axis=1, keepdims=True) * head_dim ** -0.5
        group = 16 // heads
        which = lax.shift_right_logical(iota2((16, head_dim), 0), heads.bit_length() - 1)
        if c == 0:
            loads[("k", l)].wait()

        def score(g, _):
            o = pl.multiple_of(g * 16, 16)
            qg = q_rows[pl.ds(o, 16)]
            acc = jnp.zeros((16, head_dim), F32)
            for j in range(group):
                acc = jnp.where(which == j, dot(qg, kv_all[0, l, c * cr + g * group + j], NT), acc)
            s_rows[pl.ds(o, 16)] = acc
            return 0

        lax.fori_loop(0, hr // 16, score, 0, unroll=hr // 16)
        s = s_rows[...] * head_dim ** -0.5
        pos = iota2((hr, s.shape[1]), 1).astype(F32)
        s = jnp.where(pos < len_rep[c], s, -1e30)
        top = jnp.maximum(jnp.max(s, axis=1, keepdims=True), s_new)
        w = jnp.exp(s - top)
        w_new = jnp.exp(s_new - top)
        total = jnp.sum(w, axis=1, keepdims=True) + w_new
        q_rows[...] = w.astype(BF)
        if c == 0:
            loads[("v", l)].wait()

        def mixv(g, _):
            o = pl.multiple_of(g * 16, 16)
            wg = q_rows[pl.ds(o, 16)]
            acc = jnp.zeros((16, head_dim), F32)
            for j in range(group):
                acc = jnp.where(which == j, dot(wg, kv_all[1, l, c * cr + g * group + j]), acc)
            o_rows[pl.ds(o, 16)] = acc
            return 0

        lax.fori_loop(0, hr // 16, mixv, 0, unroll=hr // 16)
        mixed = (o_rows[...] + w_new.astype(BF).astype(F32) * v_rep) / total
        back = jnp.where(ri == (ci & (heads - 1)) * cr + lax.shift_right_logical(ci, heads.bit_length() - 1), 1.0, 0.0).astype(BF)
        heads_o = dot(back, mixed.astype(BF)).astype(BF)
        for t in range(tp):
            o_send[l, c, t] = heads_o[(t // 2) * cr:(t // 2 + 1) * cr, (t % 2) * half:(t % 2 + 1) * half]
        for dev in others:
            rcopy(o_send.at[l, c, dev], o_recv.at[l, c, me], o_ss, o_rs.at[l, c], dev).start()
        o_recv[l, c, me] = o_send[l, c, me]

    def project(l, c):
        cl = pl.ds(c * cw, cw)
        got(o_recv.at[l, c, pl.ds(0, tp - 1)], o_rs.at[l, c])
        o_all = jnp.concatenate([o_recv[l, c, j].astype(F32) for j in range(tp)], axis=0)
        joined[pl.ds(ffn_dev, q_dev), cl] = jnp.transpose(o_all).astype(BF)

        for n, slot in enumerate((dd + flip, dx + flip, dy + flip, me + flip, dd, dx, dy, me)):
            at = pl.ds(pl.multiple_of(slot * shard, 16), shard)
            y_part[l, at, cl] = dot(w_out_t[at], joined[:, cl]).astype(BF)
            if n < 4:
                rcopy(y_part.at[l, at, cl], d2d.at[l, slot // 2, :, cl], d_ss.at[l], d_rs.at[l, c], dp_).start()

    def turn_out(l):
        loads[("out", l)].wait()

        def body(i, _):
            o = pl.multiple_of(i * 128, 128)
            w_out_t[pl.ds(o, 128)] = jnp.transpose(w_out_v[:, pl.ds(o, 128)])
            return 0

        lax.fori_loop(0, width // 128, body, 0)

    def chip_sum(l, c, slot, n):
        if n == 0:
            got(d2d.at[l, :, :, lanes(c)], d_rs.at[l, c])
        mine = y_part[l, pl.ds(pl.multiple_of(slot * shard, 16), shard), lanes(c)].astype(F32)
        return mine + d2d[l, slot // 2, :, lanes(c)].astype(F32)

    def rs_first(l, c):
        for n, dev in enumerate((dd, dx, dy)):
            rs_send[l, c, n] = chip_sum(l, c, dev, n).astype(BF)
            rcopy(rs_send.at[l, c, n], rs_recv.at[l, c, n], t_ss, t_rs.at[l, c], dev).start()

    def chip_sums(l, c):
        for n, (out, dev) in enumerate(((sum_d, dd), (sum_x, dx), (sum_y, dy))):
            out[:, lanes(c)] = chip_sum(l, c, dev, n).astype(BF)
        base[:, lanes(c)] = r_all[l, me, :, lanes(c)].astype(F32) + chip_sum(l, c, me, 3)

    def rs_last(l, c):
        total = chip_sum(l, c, me, 3)
        got(rs_recv.at[l, c], t_rs.at[l, c])
        for n in range(3):
            total = total + rs_recv[l, c, n].astype(F32)
        return (r_all[l, me, :, lanes(c)].astype(F32) + total).astype(BF)

    def keep(l, c, part):
        r_all[l, me, :, lanes(c)] = part
        ag_start(l, c)

    ln_start()
    ag_start(0, 0)
    ag_start(0, 1)
    load_cache(0)
    setup_angles()
    turn_out(0)
    ln_finish()
    ag_relay(0, 0)
    ag_finish(0, 0)
    for l in range(layers):
        last = l + 1 == layers
        loads[("in", l)].wait()
        norm_query(l, 0)
        if not last:
            load_cache(l + 1)
        loads[("key", l)].wait()
        loads[("val", l)].wait()
        key_value(l, 0)
        if l == 0:
            ag_relay(l, 1)
            feed_forward(l, 0)
        else:
            feed_forward(l, 0)
            ag_relay(l, 1)
        ag_finish(l, 1)
        norm_query(l, 1)
        key_value(l, 1)
        attention(l, 0)
        if not last:
            feed_forward(l, 1)
            load_in(l + 1)
            load_out(l + 1)
        attention(l, 1)
        if last:
            feed_forward(l, 1)
        project(l, 0)
        if last:
            project(l, 1)
            chip_sums(l, 0)
            chip_sums(l, 1)
        else:
            rs_first(l, 0)
            project(l, 1)
            rs_first(l, 1)
            keep(l + 1, 0, rs_last(l, 0))
            turn_out(l + 1)
            keep(l + 1, 1, rs_last(l, 1))
            ag_relay(l + 1, 0)
            ag_finish(l + 1, 0)

    def sent(ref, sem):
        rcopy(ref, ref, sem, ln_rs, dp_).wait_send()

    sent(ln_all.at[pl.ds(0, tp - 1)], ln_ss)
    sent(q_send.at[:, pl.ds(0, CHUNKS * (tp - 1) * cr)], q_ss)
    sent(o_send.at[:, :, pl.ds(0, tp - 1)], o_ss)
    for l in range(layers):
        sent(r_all.at[l, pl.ds(0, tp - 1)], ag_ss.at[l])
        sent(y_part.at[l, pl.ds(0, width // 2)], d_ss.at[l])
    sent(rs_send, t_ss)


def order(cw, cr, rows, batch):
    pos = iota2((1, batch), 1)
    want = ((pos & (cw - 1)) // cr) * rows + (pos // cw) * cr + (pos & (cr - 1))
    return jnp.where(iota2((batch, batch), 0) == want, 1.0, 0.0).astype(BF)


def final_kernel(cw, cr, rows, base, part_d, part_x, part_y, out):
    total = base[...] + part_d[...].astype(F32) + part_x[...].astype(F32) + part_y[...].astype(F32)
    out[...] = dot(total.astype(BF), order(cw, cr, rows, base.shape[1]), NT).astype(BF)


def cache_kernel(lengths, new_k, new_v, kv_all, k_out, v_out, tiles, ends, big_sems, tile_sems):
    layers, rows = kv_all.shape[1:3]
    per = 16
    pairs = [(kv_all.at[0], k_out, new_k, 0), (kv_all.at[1], v_out, new_v, 1)]
    jobs = [(l, g, pair) for l in range(layers) for pair in pairs for g in range(rows // per)]

    n_tail = ends.shape[0]
    body = len(jobs) - n_tail

    def big(i):
        l, g, (src, dst, _, _) = jobs[i]
        at = pl.ds(g * per, per)
        return pltpu.make_async_copy(src.at[l, at] if i < body else ends.at[i - body], dst.at[l, at], big_sems.at[i])

    for i in range(body):
        big(i).start()
    for i in range(body, len(jobs)):
        l, g, (src, _, new, _) = jobs[i]

        def fill(j, _):
            b = g * per + j
            slot = lengths[b]
            base = pl.multiple_of((slot // 16) * 16, 16)
            hit = iota2((16, kv_all.shape[4]), 0) == slot - base
            ends[i - body, j] = src[l, b]
            old = src[l, b, pl.ds(base, 16)].astype(F32)
            ends[i - body, j, pl.ds(base, 16)] = jnp.where(hit, new[l, pl.ds(b, 1)], old).astype(BF)
            return 0

        lax.fori_loop(0, per, fill, 0)
        big(i).start()

    def build(b, _):
        slot = lengths[b]
        base = pl.multiple_of((slot // 16) * 16, 16)
        hit = iota2((16, kv_all.shape[4]), 0) == slot - base
        for l in range(layers):
            for src, _, new, n in pairs:
                old = src[l, b, pl.ds(base, 16)].astype(F32)
                tiles[l, n, b] = jnp.where(hit, new[l, pl.ds(b, 1)], old).astype(BF)
        return 0

    lax.fori_loop(0, rows, build, 0, unroll=4)
    for i in range(body):
        l, g, (_, dst, _, n) = jobs[i]
        big(i).wait()

        def patch(j, _):
            b = g * per + j
            base = pl.multiple_of((lengths[b] // 16) * 16, 16)
            pltpu.make_async_copy(tiles.at[l, n, b], dst.at[l, b, pl.ds(base, 16)], tile_sems.at[i]).start()
            return 0

        lax.fori_loop(0, per, patch, 0, unroll=4)
    for i in range(len(jobs)):
        if i >= body:
            big(i).wait()
            continue
        l, g, (_, dst, _, n) = jobs[i]
        at = pl.ds(g * per, per)
        pltpu.make_async_copy(tiles.at[l, n, at], dst.at[l, at, pl.ds(0, 16)], tile_sems.at[i]).wait()


def solution(mesh):
    tp = mesh.shape["tp"]

    def device_step(residual, lengths, ln_scale, w_in, w_key, w_val, w_out, key_cache, val_cache):
        layers, width, in_cols = w_in.shape
        batch, shard = residual.shape
        rows = lengths.shape[0]
        head_dim = w_key.shape[2]
        ffn_dev = in_cols - w_out.shape[1]
        q_dev = w_out.shape[1] - ffn_dev
        heads = q_dev * tp // head_dim
        cw, cr = batch // CHUNKS, rows // CHUNKS
        hr = cr * heads
        slots = key_cache.shape[2]
        inv_freq = jnp.asarray((10000.0 ** (-np.arange(head_dim // 2) * (2.0 / head_dim))).astype(np.float32))[None, :]
        vmem = pl.BlockSpec(memory_space=pltpu.VMEM)
        hbm = pl.BlockSpec(memory_space=pltpu.HBM)
        smem = pl.BlockSpec(memory_space=pltpu.SMEM)
        dma = pltpu.SemaphoreType.DMA
        sum_d, sum_x, sum_y, base, new_k, new_v, kv_all = pl.pallas_call(
            step_kernel,
            out_shape=[pltpu.VMEM((shard, batch), BF)] * 3 + [
                       pltpu.VMEM((shard, batch), F32),
                       pltpu.VMEM((layers, rows, head_dim), F32),
                       pltpu.VMEM((layers, rows, head_dim), F32),
                       pltpu.VMEM((2,) + key_cache.shape, BF)],
            in_specs=[hbm] + [vmem] * 3 + [hbm] * 6,
            out_specs=[vmem] * 7,
            scratch_shapes=[
                pltpu.VMEM((in_cols, width), BF),
                pltpu.VMEM((width, head_dim), BF),
                pltpu.VMEM((width, head_dim), BF),
                pltpu.VMEM((w_out.shape[1], width), BF),
                pltpu.VMEM((width, w_out.shape[1]), BF),
                pltpu.VMEM((layers, tp, shard, batch), BF),
                pltpu.VMEM((tp, layers, shard), BF),
                pltpu.VMEM((layers, tp, shard, 128), F32),
                pltpu.VMEM((width, batch), BF),
                pltpu.VMEM((ffn_dev + q_dev, batch), BF),
                pltpu.VMEM((layers, width, batch), BF),
                pltpu.VMEM((layers, tp // 2, shard, batch), BF),
                pltpu.VMEM((layers - 1, CHUNKS, 3, shard, cw), BF),
                pltpu.VMEM((layers - 1, CHUNKS, 3, shard, cw), BF),
                pltpu.VMEM((layers, batch, q_dev), BF),
                pltpu.VMEM((layers, CHUNKS, tp, cr, q_dev), BF),
                pltpu.VMEM((layers, CHUNKS, tp, cr, q_dev), BF),
                pltpu.VMEM((layers, CHUNKS, tp, cr, q_dev), BF),
                pltpu.VMEM((hr, head_dim), BF),
                pltpu.VMEM((hr, slots), F32),
                pltpu.VMEM((hr, head_dim), F32),
                pltpu.VMEM((128, head_dim), F32),
                pltpu.VMEM((CHUNKS, cr, head_dim // 2), F32),
                pltpu.VMEM((CHUNKS, cr, head_dim // 2), F32),
                pltpu.VMEM((CHUNKS, cr, 1), F32),
                pltpu.VMEM((CHUNKS, hr, 1), F32),
                pltpu.VMEM((batch, batch), BF),
                pltpu.VMEM((shard, batch), BF),
                dma,
                dma((layers, 4)), dma((layers, 2)),
                dma, dma,
                dma((layers,)), dma((layers, CHUNKS, 4)),
                dma, dma((layers, CHUNKS)),
                dma, dma((layers, CHUNKS)),
                dma((layers,)), dma((layers, CHUNKS)),
                dma, dma((layers - 1, CHUNKS)),
            ],
            compiler_params=pltpu.CompilerParams(collective_id=0, has_side_effects=True, vmem_limit_bytes=27 * 2 ** 20),
            name="step",
        )(residual.T, lengths[None, :], ln_scale, inv_freq, jnp.swapaxes(w_in, 1, 2), w_key, w_val, w_out, key_cache, val_cache)
        def swap(value, bit):
            return lax.ppermute(value, "tp", [(i, i ^ bit) for i in range(tp)])

        parts = [swap(sum_d, 6), swap(sum_x, 2), swap(sum_y, 4)]
        keep = functools.partial(pltpu.with_memory_space_constraint, memory_space=pltpu.VMEM)
        key_out, val_out = pl.pallas_call(
            cache_kernel,
            out_shape=[jax.ShapeDtypeStruct(key_cache.shape, BF)] * 2,
            in_specs=[smem] + [vmem] * 3,
            out_specs=[hbm, hbm],
            scratch_shapes=[pltpu.VMEM((layers, 2, rows, 16, head_dim), BF), pltpu.VMEM((2, 16, slots, head_dim), BF), dma((16,)), dma((14,))],
            compiler_params=pltpu.CompilerParams(vmem_limit_bytes=9 * 2 ** 20),
            name="caches",
        )(lengths, keep(new_k), keep(new_v), keep(kv_all))
        r_new = pl.pallas_call(
            functools.partial(final_kernel, cw, cr, rows),
            out_shape=jax.ShapeDtypeStruct((shard, batch), BF),
            in_specs=[vmem] * 4,
            out_specs=vmem,
            compiler_params=pltpu.CompilerParams(vmem_limit_bytes=8 * 2 ** 20),
            name="last",
        )(keep(base), *parts)
        return r_new.T, key_out, val_out

    cache_spec = P(None, ("dp", "tp"), None, None)
    return jax.shard_map(device_step, mesh=mesh, in_specs=(P("dp", "tp"), P(("dp", "tp")), P(None, "tp"), P(None, None, "tp"), P(), P(), P(None, "tp", None), cache_spec, cache_spec), out_specs=(P("dp", "tp"), cache_spec, cache_spec), check_vma=False)
```

```python
import functools

import jax
import jax.numpy as jnp
import numpy as np
from jax import lax
from jax.experimental import pallas as pl
from jax.experimental.pallas import tpu as pltpu
from jax.sharding import PartitionSpec as P

NORM_EPS = 1e-6
MESH = pl.DeviceIdType.MESH
CHUNKS = 2
BF = jnp.bfloat16
F32 = jnp.float32
TN = (((0,), (0,)), ((), ()))
NT = (((1,), (1,)), ((), ()))


def dot(a, b, dims=None):
    if dims is None:
        return jnp.dot(a, b, preferred_element_type=F32)
    return lax.dot_general(a, b, dims, preferred_element_type=F32)


def iota2(shape, dim):
    return lax.broadcasted_iota(jnp.int32, shape, dim)


def step_kernel(r_in, len_row, ln_in, inv_freq, w_in, w_key, w_val, w_out, k_cache, v_cache,
                sum_d, sum_x, sum_y, base, new_k, new_v, kv_all,
                w_in_v, w_key_v, w_val_v, w_out_v, w_out_t,
                r_all, ln_all, ln_col, h_t, joined, y_part, d2d, rs_recv, rs_send,
                q_send, q_recv, o_send, o_recv, q_rows, s_rows, o_rows, kv_tmp,
                cos_b, sin_b, len_col, len_rep, perm, r_buf, r_sem,
                w_sems, c_sems, ln_ss, ln_rs, ag_ss, ag_rs, q_ss, q_rs, o_ss, o_rs, d_ss, d_rs, t_ss, t_rs):
    layers, width = w_in.shape[0], w_in.shape[2]
    shard, batch = r_in.shape
    tp = width // shard
    rows = batch // tp
    q_dev = q_send.shape[2]
    ffn_dev = w_out.shape[1] - q_dev
    head_dim = w_key.shape[2]
    half = head_dim // 2
    heads = q_dev * tp // head_dim
    cw = batch // CHUNKS
    cr = rows // CHUNKS
    hr = cr * heads

    me = lax.axis_index("tp")
    core, xpos, ypos = me % 2, (me // 2) % 2, me // 4
    dp_ = me + 1 - 2 * core
    dx = me + 2 - 4 * xpos
    dy = me + 4 - 8 * ypos
    dd = dx + 4 - 8 * ypos
    flip = 1 - 2 * core
    others = (dd + flip, dd, dx + flip, dy + flip, dx, dy, dp_)

    def rcopy(src, dst, ss, rs, dev):
        return pltpu.make_async_remote_copy(src_ref=src, dst_ref=dst, send_sem=ss, recv_sem=rs,
                                            device_id={"tp": dev}, device_id_type=MESH)

    barrier = pltpu.get_barrier_semaphore()
    for off in range(1, tp):
        pl.semaphore_signal(barrier, 1, device_id={"tp": (me + off) % tp}, device_id_type=MESH)

    r_load = pltpu.make_async_copy(r_in, r_buf, r_sem)
    r_load.start()

    loads = {}

    def load(name, src, dst, sem):
        loads[name] = pltpu.make_async_copy(src, dst, sem)
        loads[name].start()

    def load_in(l):
        load(("key", l), w_key.at[l], w_key_v, w_sems.at[l, 1])
        load(("val", l), w_val.at[l], w_val_v, w_sems.at[l, 2])
        load(("in", l), w_in.at[l], w_in_v, w_sems.at[l, 0])

    def load_out(l):
        load(("out", l), w_out.at[l], w_out_v, w_sems.at[l, 3])

    def load_cache(l):
        load(("k", l), k_cache.at[l], kv_all.at[0, l], c_sems.at[l, 0])
        load(("v", l), v_cache.at[l], kv_all.at[1, l], c_sems.at[l, 1])

    perm[...] = order(cw, cr, rows, batch)
    r_load.wait()
    load_out(0)
    load_in(0)
    r_all[0, me] = dot(r_buf[...], perm[...]).astype(BF)
    ln_all[me] = ln_in[...]

    pl.semaphore_wait(barrier, tp - 1)

    def lanes(c):
        return pl.ds(c * cw, cw)

    def ag_send(l, c, kind, dev, slot):
        ref = r_all.at[l, slot, :, lanes(c)]
        rcopy(ref, ref, ag_ss.at[l], ag_rs.at[l, c, kind], dev).start()

    def got(ref, sem):
        rcopy(ref, ref, ln_ss, sem, dp_).wait_recv()

    def ag_start(l, c):
        ag_send(l, c, 2, dd, me)
        ag_send(l, c, 0, dx, me)
        ag_send(l, c, 1, dy, me)
        ag_send(l, c, 3, dp_, me)

    def ag_relay(l, c):
        for n, slot in enumerate((dx, dy, dd)):
            got(r_all.at[l, slot, :, lanes(c)], ag_rs.at[l, c, n])
            ag_send(l, c, 3, dp_, slot)

    def ag_finish(l, c):
        got(r_all.at[l, pl.ds(0, tp // 2), :, lanes(c)], ag_rs.at[l, c, 3])

    def ln_start():
        for off in range(1, tp):
            rcopy(ln_all.at[me], ln_all.at[me], ln_ss, ln_rs, (me + off) % tp).start()

    def ln_finish():
        got(ln_all.at[pl.ds(0, tp - 1)], ln_rs)
        for l in range(layers):
            pick = jnp.where(iota2((layers, 128), 0) == l, 1.0, 0.0).astype(BF)
            for s in range(tp):
                ln_col[l, s] = dot(ln_all[s], pick, TN)

    def setup_angles():
        lens = len_row[...].astype(F32)
        for c in range(CHUNKS):
            own = iota2((cr, rows), 1) == iota2((cr, rows), 0) + c * cr
            lc = jnp.sum(jnp.where(own, lens, 0.0), axis=1, keepdims=True)
            len_col[c] = lc
            rep = iota2((hr, rows), 1) == lax.shift_right_logical(iota2((hr, rows), 0), heads.bit_length() - 1) + c * cr
            len_rep[c] = jnp.sum(jnp.where(rep, lens, 0.0), axis=1, keepdims=True)
            ang = lc * inv_freq[...]
            cos_b[c] = jnp.cos(ang)
            sin_b[c] = jnp.sin(ang)

    def norm_query(l, c):
        cl = pl.ds(c * cw, cw)
        total = jnp.zeros((shard, cw), F32)
        squares = jnp.zeros((shard, cw), F32)
        for s in range(tp):
            v = r_all[l, s, :, cl].astype(F32)
            total = total + v
            squares = squares + v * v
        mean = jnp.sum(total, axis=0, keepdims=True) / width
        var = jnp.sum(squares, axis=0, keepdims=True) / width - mean * mean
        inv = lax.rsqrt(var + NORM_EPS)
        for s in range(tp):
            v = r_all[l, s, :, cl].astype(F32)
            scale = ln_col[l, s]
            scale = jnp.concatenate([scale] * (cw // 128), axis=1)
            h_t[pl.ds(s * shard, shard), cl] = ((v - mean) * inv * scale).astype(BF)
        q_t = dot(w_in_v[pl.ds(2 * ffn_dev, q_dev), :], h_t[:, cl])
        q_send[l, cl] = jnp.transpose(q_t).astype(BF)
        for dev in others:
            rcopy(q_send.at[l, pl.ds(c * cw + dev * cr, cr)], q_recv.at[l, c, me], q_ss, q_rs.at[l, c], dev).start()
        q_recv[l, c, me] = q_send[l, pl.ds(pl.multiple_of(c * cw + me * cr, cr), cr)]

    def key_value(l, c):
        per = 128 // cr
        blk = h_t[:, pl.ds(pl.multiple_of(c * cw + (me // per) * 128, 128), 128)]
        here = pl.ds(pl.multiple_of((me % per) * cr, cr), cr)
        kv_tmp[...] = dot(blk, w_key_v[...], TN)
        k = kv_tmp[here].astype(BF).astype(F32)
        x1, x2 = k[:, :half], k[:, half:]
        co, si = cos_b[c], sin_b[c]
        new_k[l, pl.ds(c * cr, cr), :half] = (x1 * co - x2 * si).astype(BF).astype(F32)
        new_k[l, pl.ds(c * cr, cr), half:] = (x2 * co + x1 * si).astype(BF).astype(F32)
        kv_tmp[...] = dot(blk, w_val_v[...], TN)
        new_v[l, pl.ds(c * cr, cr)] = kv_tmp[here].astype(BF).astype(F32)

    def feed_forward(l, c):
        cl = pl.ds(c * cw, cw)
        gate = dot(w_in_v[pl.ds(0, ffn_dev)], h_t[:, cl]).astype(BF).astype(F32)
        up = dot(w_in_v[pl.ds(ffn_dev, ffn_dev)], h_t[:, cl]).astype(BF).astype(F32)
        joined[pl.ds(0, ffn_dev), cl] = (gate * jax.nn.sigmoid(gate) * up).astype(BF)

    def attention(l, c):
        got(q_recv.at[l, c, pl.ds(0, tp - 1)], q_rs.at[l, c])
        co, si = cos_b[c], sin_b[c]
        r1, r2 = [], []
        for h in range(heads):
            x1 = q_recv[l, c, 2 * h].astype(F32)
            x2 = q_recv[l, c, 2 * h + 1].astype(F32)
            r1.append((x1 * co - x2 * si).astype(BF))
            r2.append((x2 * co + x1 * si).astype(BF))
        ri, ci = iota2((hr, hr), 0), iota2((hr, hr), 1)
        mix = jnp.where(ci == (ri & (heads - 1)) * cr + lax.shift_right_logical(ri, heads.bit_length() - 1), 1.0, 0.0).astype(BF)
        q_rows[:, :half] = dot(mix, jnp.concatenate(r1, axis=0)).astype(BF)
        q_rows[:, half:] = dot(mix, jnp.concatenate(r2, axis=0)).astype(BF)
        rep = jnp.where(iota2((hr, cr), 1) == lax.shift_right_logical(iota2((hr, cr), 0), heads.bit_length() - 1), 1.0, 0.0).astype(BF)
        k_rep = dot(rep, new_k[l, pl.ds(c * cr, cr)].astype(BF))
        v_rep = dot(rep, new_v[l, pl.ds(c * cr, cr)].astype(BF))
        q_all = q_rows[...].astype(F32)
        s_new = jnp.sum(q_all * k_rep, axis=1, keepdims=True) * head_dim ** -0.5
        group = 16 // heads
        which = lax.shift_right_logical(iota2((16, head_dim), 0), heads.bit_length() - 1)
        if c == 0:
            loads[("k", l)].wait()

        def score(g, _):
            o = pl.multiple_of(g * 16, 16)
            qg = q_rows[pl.ds(o, 16)]
            acc = jnp.zeros((16, head_dim), F32)
            for j in range(group):
                acc = jnp.where(which == j, dot(qg, kv_all[0, l, c * cr + g * group + j], NT), acc)
            s_rows[pl.ds(o, 16)] = acc
            return 0

        lax.fori_loop(0, hr // 16, score, 0, unroll=hr // 16)
        s = s_rows[...] * head_dim ** -0.5
        pos = iota2((hr, s.shape[1]), 1).astype(F32)
        s = jnp.where(pos < len_rep[c], s, -1e30)
        top = jnp.maximum(jnp.max(s, axis=1, keepdims=True), s_new)
        w = jnp.exp(s - top)
        w_new = jnp.exp(s_new - top)
        total = jnp.sum(w, axis=1, keepdims=True) + w_new
        q_rows[...] = w.astype(BF)
        if c == 0:
            loads[("v", l)].wait()

        def mixv(g, _):
            o = pl.multiple_of(g * 16, 16)
            wg = q_rows[pl.ds(o, 16)]
            acc = jnp.zeros((16, head_dim), F32)
            for j in range(group):
                acc = jnp.where(which == j, dot(wg, kv_all[1, l, c * cr + g * group + j]), acc)
            o_rows[pl.ds(o, 16)] = acc
            return 0

        lax.fori_loop(0, hr // 16, mixv, 0, unroll=hr // 16)
        mixed = (o_rows[...] + w_new.astype(BF).astype(F32) * v_rep) / total
        back = jnp.where(ri == (ci & (heads - 1)) * cr + lax.shift_right_logical(ci, heads.bit_length() - 1), 1.0, 0.0).astype(BF)
        heads_o = dot(back, mixed.astype(BF)).astype(BF)
        for t in range(tp):
            o_send[l, c, t] = heads_o[(t // 2) * cr:(t // 2 + 1) * cr, (t % 2) * half:(t % 2 + 1) * half]
        for dev in others:
            rcopy(o_send.at[l, c, dev], o_recv.at[l, c, me], o_ss, o_rs.at[l, c], dev).start()
        o_recv[l, c, me] = o_send[l, c, me]

    def project(l, c):
        cl = pl.ds(c * cw, cw)
        got(o_recv.at[l, c, pl.ds(0, tp - 1)], o_rs.at[l, c])
        o_all = jnp.concatenate([o_recv[l, c, j].astype(F32) for j in range(tp)], axis=0)
        joined[pl.ds(ffn_dev, q_dev), cl] = jnp.transpose(o_all).astype(BF)

        for n, slot in enumerate((dd + flip, dx + flip, dy + flip, me + flip, dd, dx, dy, me)):
            at = pl.ds(pl.multiple_of(slot * shard, 16), shard)
            y_part[l, at, cl] = dot(w_out_t[at], joined[:, cl]).astype(BF)
            if n < 4:
                rcopy(y_part.at[l, at, cl], d2d.at[l, slot // 2, :, cl], d_ss.at[l], d_rs.at[l, c], dp_).start()

    def turn_out(l):
        loads[("out", l)].wait()

        def body(i, _):
            o = pl.multiple_of(i * 128, 128)
            w_out_t[pl.ds(o, 128)] = jnp.transpose(w_out_v[:, pl.ds(o, 128)])
            return 0

        lax.fori_loop(0, width // 128, body, 0)

    def chip_sum(l, c, slot, n):
        if n == 0:
            got(d2d.at[l, :, :, lanes(c)], d_rs.at[l, c])
        mine = y_part[l, pl.ds(pl.multiple_of(slot * shard, 16), shard), lanes(c)].astype(F32)
        return mine + d2d[l, slot // 2, :, lanes(c)].astype(F32)

    def rs_first(l, c):
        for n, dev in enumerate((dd, dx, dy)):
            rs_send[l, c, n] = chip_sum(l, c, dev, n).astype(BF)
            rcopy(rs_send.at[l, c, n], rs_recv.at[l, c, n], t_ss, t_rs.at[l, c], dev).start()

    def chip_sums(l, c):
        for n, (out, dev) in enumerate(((sum_d, dd), (sum_x, dx), (sum_y, dy))):
            out[:, lanes(c)] = chip_sum(l, c, dev, n).astype(BF)
        base[:, lanes(c)] = r_all[l, me, :, lanes(c)].astype(F32) + chip_sum(l, c, me, 3)

    def rs_last(l, c):
        total = chip_sum(l, c, me, 3)
        got(rs_recv.at[l, c], t_rs.at[l, c])
        for n in range(3):
            total = total + rs_recv[l, c, n].astype(F32)
        return (r_all[l, me, :, lanes(c)].astype(F32) + total).astype(BF)

    def keep(l, c, part):
        r_all[l, me, :, lanes(c)] = part
        ag_start(l, c)

    ln_start()
    ag_start(0, 0)
    ag_start(0, 1)
    load_cache(0)
    setup_angles()
    turn_out(0)
    ln_finish()
    ag_relay(0, 0)
    ag_finish(0, 0)
    for l in range(layers):
        last = l + 1 == layers
        loads[("in", l)].wait()
        norm_query(l, 0)
        if not last:
            load_cache(l + 1)
        loads[("key", l)].wait()
        loads[("val", l)].wait()
        key_value(l, 0)
        if l == 0:
            ag_relay(l, 1)
            feed_forward(l, 0)
        else:
            feed_forward(l, 0)
            ag_relay(l, 1)
        ag_finish(l, 1)
        norm_query(l, 1)
        key_value(l, 1)
        attention(l, 0)
        if not last:
            feed_forward(l, 1)
            load_in(l + 1)
            load_out(l + 1)
        attention(l, 1)
        if last:
            feed_forward(l, 1)
        project(l, 0)
        if last:
            project(l, 1)
            chip_sums(l, 0)
            chip_sums(l, 1)
        else:
            rs_first(l, 0)
            project(l, 1)
            rs_first(l, 1)
            keep(l + 1, 0, rs_last(l, 0))
            turn_out(l + 1)
            keep(l + 1, 1, rs_last(l, 1))
            ag_relay(l + 1, 0)
            ag_finish(l + 1, 0)

    def sent(ref, sem):
        rcopy(ref, ref, sem, ln_rs, dp_).wait_send()

    sent(ln_all.at[pl.ds(0, tp - 1)], ln_ss)
    sent(q_send.at[:, pl.ds(0, CHUNKS * (tp - 1) * cr)], q_ss)
    sent(o_send.at[:, :, pl.ds(0, tp - 1)], o_ss)
    for l in range(layers):
        sent(r_all.at[l, pl.ds(0, tp - 1)], ag_ss.at[l])
        sent(y_part.at[l, pl.ds(0, width // 2)], d_ss.at[l])
    sent(rs_send, t_ss)


def order(cw, cr, rows, batch):
    pos = iota2((1, batch), 1)
    want = ((pos & (cw - 1)) // cr) * rows + (pos // cw) * cr + (pos & (cr - 1))
    return jnp.where(iota2((batch, batch), 0) == want, 1.0, 0.0).astype(BF)


def final_kernel(cw, cr, rows, base, part_d, part_x, part_y, out):
    total = base[...] + part_d[...].astype(F32) + part_x[...].astype(F32) + part_y[...].astype(F32)
    out[...] = dot(total.astype(BF), order(cw, cr, rows, base.shape[1]), NT).astype(BF)


def cache_kernel(lengths, new_k, new_v, kv_all, k_out, v_out, tiles, ends, big_sems, tile_sems):
    layers, rows = kv_all.shape[1:3]
    per = 16
    pairs = [(kv_all.at[0], k_out, new_k, 0), (kv_all.at[1], v_out, new_v, 1)]
    jobs = [(l, g, pair) for l in range(layers) for pair in pairs for g in range(rows // per)]

    n_tail = ends.shape[0]
    body = len(jobs) - n_tail

    def big(i):
        l, g, (src, dst, _, _) = jobs[i]
        at = pl.ds(g * per, per)
        return pltpu.make_async_copy(src.at[l, at] if i < body else ends.at[i - body], dst.at[l, at], big_sems.at[i])

    for i in range(body):
        big(i).start()
    for i in range(body, len(jobs)):
        l, g, (src, _, new, _) = jobs[i]

        def fill(j, _):
            b = g * per + j
            slot = lengths[b]
            base = pl.multiple_of((slot // 16) * 16, 16)
            hit = iota2((16, kv_all.shape[4]), 0) == slot - base
            ends[i - body, j] = src[l, b]
            old = src[l, b, pl.ds(base, 16)].astype(F32)
            ends[i - body, j, pl.ds(base, 16)] = jnp.where(hit, new[l, pl.ds(b, 1)], old).astype(BF)
            return 0

        lax.fori_loop(0, per, fill, 0)
        big(i).start()

    def build(b, _):
        slot = lengths[b]
        base = pl.multiple_of((slot // 16) * 16, 16)
        hit = iota2((16, kv_all.shape[4]), 0) == slot - base
        for l in range(layers):
            for src, _, new, n in pairs:
                old = src[l, b, pl.ds(base, 16)].astype(F32)
                tiles[l, n, b] = jnp.where(hit, new[l, pl.ds(b, 1)], old).astype(BF)
        return 0

    lax.fori_loop(0, rows, build, 0, unroll=4)
    for i in range(body):
        l, g, (_, dst, _, n) = jobs[i]
        big(i).wait()

        def patch(j, _):
            b = g * per + j
            base = pl.multiple_of((lengths[b] // 16) * 16, 16)
            pltpu.make_async_copy(tiles.at[l, n, b], dst.at[l, b, pl.ds(base, 16)], tile_sems.at[i]).start()
            return 0

        lax.fori_loop(0, per, patch, 0, unroll=4)
    for i in range(len(jobs)):
        if i >= body:
            big(i).wait()
            continue
        l, g, (_, dst, _, n) = jobs[i]
        at = pl.ds(g * per, per)
        pltpu.make_async_copy(tiles.at[l, n, at], dst.at[l, at, pl.ds(0, 16)], tile_sems.at[i]).wait()


def solution(mesh):
    tp = mesh.shape["tp"]

    def device_step(residual, lengths, ln_scale, w_in, w_key, w_val, w_out, key_cache, val_cache):
        layers, width, in_cols = w_in.shape
        batch, shard = residual.shape
        rows = lengths.shape[0]
        head_dim = w_key.shape[2]
        ffn_dev = in_cols - w_out.shape[1]
        q_dev = w_out.shape[1] - ffn_dev
        heads = q_dev * tp // head_dim
        cw, cr = batch // CHUNKS, rows // CHUNKS
        hr = cr * heads
        slots = key_cache.shape[2]
        inv_freq = jnp.asarray((10000.0 ** (-np.arange(head_dim // 2) * (2.0 / head_dim))).astype(np.float32))[None, :]
        vmem = pl.BlockSpec(memory_space=pltpu.VMEM)
        hbm = pl.BlockSpec(memory_space=pltpu.HBM)
        smem = pl.BlockSpec(memory_space=pltpu.SMEM)
        dma = pltpu.SemaphoreType.DMA
        sum_d, sum_x, sum_y, base, new_k, new_v, kv_all = pl.pallas_call(
            step_kernel,
            out_shape=[pltpu.VMEM((shard, batch), BF)] * 3 + [
                       pltpu.VMEM((shard, batch), F32),
                       pltpu.VMEM((layers, rows, head_dim), F32),
                       pltpu.VMEM((layers, rows, head_dim), F32),
                       pltpu.VMEM((2,) + key_cache.shape, BF)],
            in_specs=[hbm] + [vmem] * 3 + [hbm] * 6,
            out_specs=[vmem] * 7,
            scratch_shapes=[
                pltpu.VMEM((in_cols, width), BF),
                pltpu.VMEM((width, head_dim), BF),
                pltpu.VMEM((width, head_dim), BF),
                pltpu.VMEM((w_out.shape[1], width), BF),
                pltpu.VMEM((width, w_out.shape[1]), BF),
                pltpu.VMEM((layers, tp, shard, batch), BF),
                pltpu.VMEM((tp, layers, shard), BF),
                pltpu.VMEM((layers, tp, shard, 128), F32),
                pltpu.VMEM((width, batch), BF),
                pltpu.VMEM((ffn_dev + q_dev, batch), BF),
                pltpu.VMEM((layers, width, batch), BF),
                pltpu.VMEM((layers, tp // 2, shard, batch), BF),
                pltpu.VMEM((layers - 1, CHUNKS, 3, shard, cw), BF),
                pltpu.VMEM((layers - 1, CHUNKS, 3, shard, cw), BF),
                pltpu.VMEM((layers, batch, q_dev), BF),
                pltpu.VMEM((layers, CHUNKS, tp, cr, q_dev), BF),
                pltpu.VMEM((layers, CHUNKS, tp, cr, q_dev), BF),
                pltpu.VMEM((layers, CHUNKS, tp, cr, q_dev), BF),
                pltpu.VMEM((hr, head_dim), BF),
                pltpu.VMEM((hr, slots), F32),
                pltpu.VMEM((hr, head_dim), F32),
                pltpu.VMEM((128, head_dim), F32),
                pltpu.VMEM((CHUNKS, cr, head_dim // 2), F32),
                pltpu.VMEM((CHUNKS, cr, head_dim // 2), F32),
                pltpu.VMEM((CHUNKS, cr, 1), F32),
                pltpu.VMEM((CHUNKS, hr, 1), F32),
                pltpu.VMEM((batch, batch), BF),
                pltpu.VMEM((shard, batch), BF),
                dma,
                dma((layers, 4)), dma((layers, 2)),
                dma, dma,
                dma((layers,)), dma((layers, CHUNKS, 4)),
                dma, dma((layers, CHUNKS)),
                dma, dma((layers, CHUNKS)),
                dma((layers,)), dma((layers, CHUNKS)),
                dma, dma((layers - 1, CHUNKS)),
            ],
            compiler_params=pltpu.CompilerParams(collective_id=0, has_side_effects=True, vmem_limit_bytes=27 * 2 ** 20),
            name="step",
        )(residual.T, lengths[None, :], ln_scale, inv_freq, jnp.swapaxes(w_in, 1, 2), w_key, w_val, w_out, key_cache, val_cache)
        def swap(value, bit):
            return lax.ppermute(value, "tp", [(i, i ^ bit) for i in range(tp)])

        parts = [swap(sum_d, 6), swap(sum_x, 2), swap(sum_y, 4)]
        keep = functools.partial(pltpu.with_memory_space_constraint, memory_space=pltpu.VMEM)
        key_out, val_out = pl.pallas_call(
            cache_kernel,
            out_shape=[jax.ShapeDtypeStruct(key_cache.shape, BF)] * 2,
            in_specs=[smem] + [vmem] * 3,
            out_specs=[hbm, hbm],
            scratch_shapes=[pltpu.VMEM((layers, 2, rows, 16, head_dim), BF), pltpu.VMEM((8, 16, slots, head_dim), BF), dma((16,)), dma((8,))],
            compiler_params=pltpu.CompilerParams(vmem_limit_bytes=21 * 2 ** 20),
            name="caches",
        )(lengths, keep(new_k), keep(new_v), keep(kv_all))
        r_new = pl.pallas_call(
            functools.partial(final_kernel, cw, cr, rows),
            out_shape=jax.ShapeDtypeStruct((shard, batch), BF),
            in_specs=[vmem] * 4,
            out_specs=vmem,
            compiler_params=pltpu.CompilerParams(vmem_limit_bytes=8 * 2 ** 20),
            name="last",
        )(keep(base), *parts)
        return r_new.T, key_out, val_out

    cache_spec = P(None, ("dp", "tp"), None, None)
    return jax.shard_map(device_step, mesh=mesh, in_specs=(P("dp", "tp"), P(("dp", "tp")), P(None, "tp"), P(None, None, "tp"), P(), P(), P(None, "tp", None), cache_spec, cache_spec), out_specs=(P("dp", "tp"), cache_spec, cache_spec), check_vma=False)
```
